32 devices in a mesh: expert: 16 (over z, y, x), etp: 2 (over core).
Axes of the slice: x: 2, y: 2, z: 4, core: 2. Of those that a mesh axis runs over, the one named last changes fastest.
Arguments:
- grad_out: bfloat16 [2048, 3584], P('expert', 'etp'), may hold values from -6 to 6
- combine: bfloat16 [2048, 8], P('expert'), may hold values from 0.099609375 to 2.5
- expert_ids: int32 [2048, 8], P('expert'), may hold values from 0 to 31, all different within a row; in each aligned block of 128 rows (0 to 127, 128 to 255, ...) at most 64 rows name the same one
- saved_gate: bfloat16 [1024, 32, 1024], P(None, 'expert', 'etp'), may hold values from -6 to 6
- saved_up: bfloat16 [1024, 32, 1024], P(None, 'expert', 'etp'), may hold values from -1.5 to 1.5
- gate_weight: bfloat16 [32, 3584, 1024], P('expert', None, 'etp'), may hold values from -0.09375 to 0.09375
- up_weight: bfloat16 [32, 3584, 1024], P('expert', None, 'etp'), may hold values from -0.09375 to 0.09375
- down_weight: bfloat16 [32, 1024, 3584], P('expert', 'etp'), may hold values from -0.09375 to 0.09375
Outputs:
- grad_tokens: bfloat16 [2048, 3584], P('expert', 'etp')
- grad_combine: bfloat16 [2048, 8], P('expert')
The draws below stay inside these ranges and needn't reach their ends.
Inputs may be any that keep to these rules, and one draw needn't show every extreme that they name: `expert_ids`: each token names 8 different experts. Among the 128 tokens of one block (one index of expert), at most 64 name any one expert, and some blocks reach that bound.
All inputs are finite; a program needn't handle non-finite values.
Results may differ from the reference program's by a relative error of at most 0.012.
Values may be sent and summed in bfloat16 or wider, within the bound.
A program may use at most 192 MiB of HBM per device.

```python
import math
import jax
import jax.numpy as jnp
import numpy as np
from jax import lax

D = 3584
FF = 1024
TOP = 8
TOK_DEV = 128
EXPERTS = 32
TOKENS = 2048
CAP = 64
SLOT_ROWS = 1024
N_EXPERT = 16
N_ETP = 2


def steps_of(stream_key, extent, shards, smallest, top_value):
    gain = 1.0
    for axis_at, parts in shards:
        draws = jax.random.uniform(jax.random.fold_in(jax.random.fold_in(stream_key, 6), axis_at), (parts,), jnp.float32, smallest / len(shards), top_value / len(shards))
        gain = gain * jnp.repeat(jnp.exp(draws), extent[axis_at] // parts).reshape((-1,) + (1,) * (len(extent) - 1 - axis_at))
    return gain


def shared_out(rng, own, number, rows, amount, top, limit, slope):
    sequence = jax.random.permutation(rng, amount)
    crowded, ordinary = portions_of(amount, rows * top, limit, slope, True), portions_of(amount, rows * top, limit, slope, False)
    places = jnp.arange(amount)

    def named(sizes, rotation):
        used = int((sizes > 0).sum())
        fixed = max(1, used // 4)
        passed = fixed + (places - fixed + rotation * (used - fixed)) % max(1, amount - fixed)
        return jnp.zeros((amount,), jnp.int32).at[sequence[jnp.where(places < fixed, places, passed)]].set(jnp.asarray(sizes, jnp.int32))

    sizes = jnp.where(number % 4 == 0, named(crowded, number // 4), named(ordinary, number - number // 4 - 1))
    mixed = jax.random.permutation(jax.random.fold_in(own, 3), amount)
    source_of, taker = mixed[0:amount // 2 * 2:2], mixed[1:amount // 2 * 2:2]
    room = jnp.minimum(sizes[source_of] - 1, limit - sizes[taker]) // 2
    room = jnp.where((source_of == sequence[0]) | (taker == sequence[0]) | (sizes[taker] == 0), 0, jnp.maximum(room, 0))
    passed = jax.random.randint(jax.random.fold_in(own, 4), (amount // 2,), 0, 1 << 20) % (room + 1)
    sizes = sizes.at[source_of].add(-passed).at[taker].add(passed)
    labels = jnp.searchsorted(jnp.cumsum(sizes), jnp.arange(rows * top), side="right").astype(jnp.int32)
    grid = labels.reshape(top, rows).T
    grid = grid[jax.random.permutation(jax.random.fold_in(own, 1), rows)]
    rotation = jax.random.randint(jax.random.fold_in(own, 2), (rows, 1), 0, top)
    return jnp.take_along_axis(grid, (jnp.arange(top)[None, :] + rotation) % top, axis=1)


def portions_of(count, total, bound, slope, full):
    loads = [(1 << 20) // math.isqrt(standing ** slope) + 1 for standing in range(1, count + 1)]
    largest = bound if full else min(bound, max(-(-total // count), total * loads[0] // sum(loads)))
    least = 1 if total - largest >= count - 1 else 0
    given, spare = [largest] + [least] * (count - 1), total - largest - least * (count - 1)
    while spare > 0:
        free = [i for i in range(1, count) if given[i] < largest] or [i for i in range(1, count) if given[i] < bound]
        whole, remaining = sum([loads[i] for i in free]), spare
        for i in free:
            more = min(bound - given[i], max(1, remaining * loads[i] // whole), spare)
            given[i] = given[i] + more
            spare = spare - more
    return np.array(given)


def gaussian(key, extent, spread, most, cuts=(), held_as=jnp.bfloat16):
    level = steps_of(key, extent, cuts, -0.22, 0.18) if cuts else 1.0
    drawn = jax.random.normal(key, extent, jnp.float32) * spread * level
    return jnp.minimum(jnp.maximum(drawn, -most), most).astype(held_as)


def setup_inputs(seed: int = 0) -> dict:
    keys = jax.random.split(jax.random.key(seed), 9)
    grad_out = gaussian(keys[0], (TOKENS, D), 1.0, 6.0, ((0, 16), (1, 2)))
    combine = jnp.clip(jnp.exp(math.log(2.5) - 3.2227897 * jax.random.uniform(keys[1], (TOKENS, TOP), jnp.float32) ** steps_of(keys[1], (TOKENS, TOP), ((0, 16),), -0.2, 0.2)), 0.099609375, 2.5).astype(jnp.bfloat16)
    expert_ids_keys = jax.random.split(jax.random.fold_in(keys[2], 1), TOKENS // TOK_DEV)
    expert_ids_turns = jax.random.permutation(jax.random.fold_in(keys[2], 3), TOKENS // TOK_DEV)
    expert_ids = jax.vmap(lambda own, number: shared_out(jax.random.fold_in(keys[2], 2), own, number, TOK_DEV, EXPERTS, TOP, CAP, 2))(expert_ids_keys, expert_ids_turns).reshape((TOKENS, TOP))
    saved_gate = gaussian(keys[3], (SLOT_ROWS, EXPERTS, FF), 1.0, 6.0, ((1, 16), (2, 2)))
    saved_up = gaussian(keys[4], (SLOT_ROWS, EXPERTS, FF), 0.1, 1.5, ((1, 16), (2, 2)))
    gate_weight = gaussian(keys[5], (EXPERTS, D, FF), D ** -0.5, 0.09375, ((0, 16), (2, 2)))
    up_weight = gaussian(keys[6], (EXPERTS, D, FF), D ** -0.5, 0.09375, ((0, 16), (2, 2)))
    down_weight = gaussian(keys[7], (EXPERTS, FF, D), D ** -0.5, 0.09375, ((0, 16), (1, 2)))
    return dict(grad_out=grad_out, combine=combine, expert_ids=expert_ids, saved_gate=saved_gate, saved_up=saved_up, gate_weight=gate_weight, up_weight=up_weight, down_weight=down_weight)


def reference(grad_out, combine, expert_ids, saved_gate, saved_up, gate_weight, up_weight, down_weight):
    token_total, top_count = expert_ids.shape
    experts, model_width, hidden = gate_weight.shape
    groups = N_EXPERT
    token_count = token_total // groups
    capacity = saved_gate.shape[0] // groups
    slot_total = groups * capacity
    grouped = expert_ids.reshape(groups, token_count, top_count)
    matches = grouped[..., None] == jnp.arange(experts, dtype=jnp.int32)
    expert_loads = jnp.sum(matches.astype(jnp.int32), axis=2)
    earlier = jnp.cumsum(expert_loads, axis=1) - expert_loads
    position = jnp.sum(jnp.where(matches, earlier[:, :, None, :], 0), axis=3)
    row_index = (jnp.arange(groups, dtype=jnp.int32)[:, None, None] * capacity + position).reshape(token_total, top_count)
    slot_owner = jnp.full((slot_total, experts), token_total * top_count, jnp.int32)
    slot_owner = slot_owner.at[row_index.reshape(-1), expert_ids.reshape(-1)].set(
        jnp.arange(token_total * top_count, dtype=jnp.int32))
    grad_padded = jnp.concatenate([grad_out, jnp.zeros((1, model_width), jnp.bfloat16)], axis=0)
    weight_padded = jnp.concatenate([combine.reshape(-1).astype(jnp.float32), jnp.zeros((1,), jnp.float32)])
    half_hidden = hidden // N_ETP

    def per_expert(running, expert):
        grad_acc, weight_acc = running
        slot_ids = lax.dynamic_index_in_dim(slot_owner, expert, 1, keepdims=False)
        token_of = slot_ids // top_count
        slot_rows = jnp.take(grad_padded, token_of, axis=0)
        slot_weight = jnp.take(weight_padded, slot_ids, axis=0)
        gate_value = lax.dynamic_index_in_dim(saved_gate, expert, 1, keepdims=False).astype(jnp.float32)
        up_value = lax.dynamic_index_in_dim(saved_up, expert, 1, keepdims=False).astype(jnp.float32)
        down_expert = lax.dynamic_index_in_dim(down_weight, expert, 0, keepdims=False)
        gate_expert = lax.dynamic_index_in_dim(gate_weight, expert, 0, keepdims=False)
        up_expert = lax.dynamic_index_in_dim(up_weight, expert, 0, keepdims=False)
        grad_hidden = jnp.dot(slot_rows, down_expert.T, preferred_element_type=jnp.float32)
        gate_sigmoid = jax.nn.sigmoid(gate_value)
        activated = gate_value * gate_sigmoid
        product = grad_hidden * activated * up_value
        weight_halves = jnp.sum(product.reshape(slot_total, N_ETP, half_hidden), axis=2).astype(jnp.bfloat16)
        weight_halves = lax.optimization_barrier(weight_halves).astype(jnp.float32)
        slot_dw = jnp.sum(weight_halves, axis=1).astype(jnp.bfloat16)
        scaled = slot_weight[:, None] * grad_hidden
        grad_gate = (scaled * up_value * gate_sigmoid * (1.0 + gate_value * (1.0 - gate_sigmoid))).astype(jnp.bfloat16)
        grad_up = (scaled * activated).astype(jnp.bfloat16)
        running_sum = jnp.zeros((slot_total, model_width), jnp.float32)
        for half_index in range(N_ETP):
            lower = half_index * half_hidden
            term_half = jnp.dot(grad_gate[:, lower:lower + half_hidden], gate_expert[:, lower:lower + half_hidden].T,
                                preferred_element_type=jnp.float32)
            term_half = term_half + jnp.dot(grad_up[:, lower:lower + half_hidden], up_expert[:, lower:lower + half_hidden].T,
                                            preferred_element_type=jnp.float32)
            term_half = lax.optimization_barrier(term_half.astype(jnp.bfloat16))
            running_sum = running_sum + term_half.astype(jnp.float32)
        slot_grad = running_sum.astype(jnp.bfloat16)
        grad_acc = grad_acc.at[token_of].add(slot_grad.astype(jnp.float32), mode="drop")
        weight_acc = weight_acc.at[slot_ids].set(slot_dw.astype(jnp.float32), mode="drop")
        return (grad_acc, weight_acc), None

    start = (jnp.zeros((token_total, model_width), jnp.float32), jnp.zeros((token_total * top_count,), jnp.float32))
    final, _ = lax.scan(per_expert, start, jnp.arange(experts, dtype=jnp.int32))
    grad_tokens = final[0].astype(jnp.bfloat16)
    grad_combine = final[1].reshape(token_total, top_count).astype(jnp.bfloat16)
    return grad_tokens, grad_combine
```

```python
import functools

import jax
import jax.numpy as jnp
from jax import lax
from jax.experimental import pallas as pl
from jax.experimental.pallas import tpu as pltpu
from jax.sharding import PartitionSpec as P

MESH = pl.DeviceIdType.MESH
VMEM_LIMIT = 66_000_000
TOKEN_BYTES = 24 * 2**20
NT = (((1,), (1,)), ((), ()))
TN = (((0,), (0,)), ((), ()))
ROWS = 8


def dot_nt(a, b):
    return lax.dot_general(a, b, NT, preferred_element_type=jnp.float32)


def place():
    e = lax.axis_index("expert")
    c = lax.axis_index("etp")
    return e, c, e // 4, (e // 2) % 2, e % 2


def index(z, y, x):
    return z * 4 + y * 2 + x


def enter(groups, e, c):
    barrier = pltpu.get_barrier_semaphore()

    @pl.loop(1, groups)
    def _(i):
        pl.semaphore_signal(
            barrier, inc=1, device_id=(lax.rem(e + i, groups), c), device_id_type=MESH
        )

    pl.semaphore_signal(barrier, inc=1, device_id=(e, 1 - c), device_id_type=MESH)
    pl.semaphore_wait(barrier, groups)


def remote(src, dst, send, recv, expert, core):
    return pltpu.make_async_remote_copy(
        src_ref=src,
        dst_ref=dst,
        send_sem=send,
        recv_sem=recv,
        device_id=(expert, core),
        device_id_type=MESH,
    )


def one_hot(slot_row, capacity):
    tokens = slot_row.shape[1]
    at = lax.broadcasted_iota(jnp.int32, (capacity, tokens), 0).astype(jnp.float32)
    return jnp.where(slot_row == at, 1.0, 0.0)


def dispatch_kernel(
    nz, capacity,
    x_hbm, weights_ref, down_hbm, gate_ref, up_ref,
    hidden_ref, slot_ref, part_ref,
    own, other, weights, down, rows_own, rows_other, scale,
    load_sem, sx, rx, sy, ry, su, sd, rz, sc, rc, sw, rw,
):
    e, c, z, y, x = place()
    groups = nz * 4
    per_group, hidden, _ = down.shape
    tokens = weights.shape[2]
    features = own.shape[3]
    half = tokens // 2
    width = 256
    pieces = hidden // width
    beside, above = index(z, y, 1 - x), index(z, 1 - y, x)

    load_x = pltpu.make_async_copy(x_hbm, own.at[e], load_sem.at[0])
    load_x.start()
    load_down = pltpu.make_async_copy(down_hbm, down, load_sem.at[1])
    load_down.start()
    weights[e] = weights_ref[e]
    enter(groups, e, c)
    load_x.wait()

    def along_x(b, h, p, slot):
        return remote(own.at[b, h], own.at[b, h], sx.at[p, slot], rx.at[p, slot], beside, c)

    def along_y(b, h, p, slot):
        return remote(own.at[b, h], own.at[b, h], sy.at[p, slot], ry.at[p, slot], above, c)

    def along_z(p, h, up):
        b = index(p, y, x)
        to = e + 4 if up else e - 4
        return remote(own.at[b, h], own.at[b, h], (su if up else sd).at[p, h], rz.at[p, h], to, c)

    def cross(b):
        return remote(own.at[b], other.at[b], sc.at[b], rc.at[b], e, 1 - c)

    def plane_send(p):
        b = index(p, y, x)
        along_x(b, 0, p, 0).start()
        along_y(b, 1, p, 1).start()
        along_x(b, 1, p, 1).start()
        along_y(b, 0, p, 0).start()

    def order(k):
        low = jnp.where(k <= z, z - k, k)
        back = nz - 1 - z
        high = jnp.where(k <= back, z + k, nz - 1 - k)
        return jnp.where(z < nz // 2, low, high)

    plane_send(z)

    @pl.when(z < nz - 1)
    def _():
        for h in range(2):
            along_z(z, h, True).start()

    @pl.when(z > 0)
    def _():
        for h in range(2):
            along_z(z, h, False).start()

    cross(e).start()

    def tile(i):
        to = lax.rem(e + i, groups)
        return remote(weights_ref.at[to], weights.at[e], sw.at[i], rw.at[i], to, c)

    @pl.loop(1, groups)
    def _(i):
        tile(i).start()

    @pl.loop(1, groups)
    def _(i):
        tile(i).wait_recv()

    named = (weights[...] > 0).astype(jnp.bfloat16).reshape(groups * ROWS, tokens)
    first = lax.broadcasted_iota(jnp.int32, (tokens, tokens), 0)
    second = lax.broadcasted_iota(jnp.int32, (tokens, tokens), 1)
    before = (first < second).astype(jnp.bfloat16)
    position = jnp.dot(named, before, preferred_element_type=jnp.float32)
    slot_ref[...] = jnp.where(named > 0, position, -1.0).reshape(groups, ROWS, tokens)
    part_ref[...] = jnp.zeros_like(part_ref)
    load_down.wait()

    own_at = pl.multiple_of(c * features, 128)
    other_at = pl.multiple_of((1 - c) * features, 128)

    def gather(b, q):
        slots = slot_ref[b]
        table = weights[b]
        picks = []
        for l in range(per_group):
            pick = one_hot(slots[l : l + 1], capacity)
            amount = jnp.sum(pick * table[l : l + 1], axis=1, keepdims=True)
            scale[l, pl.ds(q * capacity, capacity)] = jnp.broadcast_to(amount, (capacity, 128))
            picks.append(pick)
        pick = jnp.concatenate(picks, axis=0).astype(jnp.bfloat16)
        for held, rows in ((own, rows_own), (other, rows_other)):
            block = held[b].reshape(tokens, features)
            got = jnp.dot(pick, block, preferred_element_type=jnp.float32).astype(jnp.bfloat16)
            for l in range(per_group):
                rows[l, pl.ds(q * capacity, capacity)] = got[l * capacity : (l + 1) * capacity]

    def hidden_grads(p, l):
        count = 4 * capacity
        at = pl.ds(pl.multiple_of(p * count, count), count)
        weight_part = jnp.zeros((count, 1), jnp.float32)
        for j in range(pieces):
            cut = slice(j * width, (j + 1) * width)
            grad = dot_nt(rows_own[l], down[l, cut, pl.ds(own_at, features)])
            grad = grad + dot_nt(rows_other[l], down[l, cut, pl.ds(other_at, features)])
            gate = gate_ref[l, at, cut].astype(jnp.float32)
            up = up_ref[l, at, cut].astype(jnp.float32)
            sigmoid = jax.nn.sigmoid(gate)
            active = gate * sigmoid
            weight_part = weight_part + jnp.sum(grad * active * up, axis=1, keepdims=True)
            scaled = scale[l][:, :1] * grad
            grad_gate = scaled * up * sigmoid * (1.0 + gate * (1.0 - sigmoid))
            hidden_ref[l, at, cut] = grad_gate.astype(jnp.bfloat16)
            cut = slice(hidden + j * width, hidden + (j + 1) * width)
            hidden_ref[l, at, cut] = (scaled * active).astype(jnp.bfloat16)
        weight_part = weight_part.astype(jnp.bfloat16).astype(jnp.float32)
        for q in range(4):
            b = p * 4 + q
            pick = one_hot(slot_ref[b, pl.ds(l, 1)], capacity)
            piece = weight_part[q * capacity : (q + 1) * capacity]
            part_ref[b, pl.ds(l, 1)] = jnp.sum(pick * piece, axis=0, keepdims=True)

    @pl.loop(0, nz)
    def _(k):
        p = order(k)
        mine = index(p, y, x)
        side, over = index(p, y, 1 - x), index(p, 1 - y, x)
        corner = index(p, 1 - y, 1 - x)
        along_x(side, 0, p, 0).wait_recv()
        along_y(side, 0, p, 2).start()
        along_y(over, 1, p, 1).wait_recv()
        along_x(over, 1, p, 2).start()

        far = k + 1

        @pl.when(z - far >= 0)
        def _():
            for h in range(2):
                along_z(z - far, h, True).wait_recv()

                @pl.when(z < nz - 1)
                def _():
                    along_z(z - far, h, True).start()

        @pl.when(z + far < nz)
        def _():
            for h in range(2):
                along_z(z + far, h, False).wait_recv()

                @pl.when(z > 0)
                def _():
                    along_z(z + far, h, False).start()

        @pl.when(far < nz)
        def _():
            after = order(far)
            plane_send(after)
            cross(index(after, y, x)).start()

        along_x(side, 1, p, 1).wait_recv()
        cross(side).start()
        along_y(over, 0, p, 0).wait_recv()
        cross(over).start()
        along_y(corner, 0, p, 2).wait_recv()
        along_x(corner, 1, p, 2).wait_recv()
        cross(corner).start()

        @pl.loop(0, 4)
        def _(i):
            q = lax.rem(i + y * 2 + x, 4)
            cross(p * 4 + i).wait_recv()

        @pl.loop(0, 4)
        def _(q):
            gather(p * 4 + q, q)

        @pl.loop(0, per_group)
        def _(l):
            hidden_grads(p, l)

    @pl.loop(0, nz)
    def _(p):
        for slot in range(3):
            along_x(e, 0, p, slot).wait_send()
            along_y(e, 0, p, slot).wait_send()

        @pl.when((p <= z) & (z < nz - 1))
        def _():
            for h in range(2):
                along_z(p, h, True).wait_send()

        @pl.when((p >= z) & (z > 0))
        def _():
            for h in range(2):
                along_z(p, h, False).wait_send()

    @pl.loop(0, groups)
    def _(b):
        cross(b).wait_send()

    @pl.loop(1, groups)
    def _(i):
        tile(i).wait_send()


def combine_kernel(
    nz, capacity,
    hidden_hbm, slot_ref, part_ref, gate_hbm, up_hbm,
    out_ref, part_out,
    hid, gate, up, partial, mine_buf, send_buf, peer, from_x, from_y, from_z, part_peer, part_sum,
    load_sem, sx, rx, sy, ry, sz, rz, sc, rc, sw, rw, sp, rp,
):
    e, c, z, y, x = place()
    groups = nz * 4
    per_group, model, hidden = gate.shape
    tokens = slot_ref.shape[2]
    features = mine_buf.shape[3]
    half = tokens // 2
    width = 512 if model % 512 == 0 else 256
    beside, above = index(z, y, 1 - x), index(z, 1 - y, x)

    loads = []
    for l in range(per_group):
        for i, (src, dst) in enumerate(((hidden_hbm, hid), (gate_hbm, gate), (up_hbm, up))):
            copy = pltpu.make_async_copy(src.at[l], dst.at[l], load_sem.at[l, i])
            copy.start()
            loads.append(copy)
    enter(groups, e, c)
    part_copy = remote(part_ref, part_peer, sp, rp, e, 1 - c)
    part_copy.start()

    def order(k):
        low = jnp.where(k < nz - 1 - z, nz - 1 - k, k - (nz - 1 - z))
        high = jnp.where(k < z, k, nz - 1 - (k - z))
        p = jnp.where(z < nz // 2, low, high)
        return jnp.where(k == nz - 1, z, p)

    def cross(b):
        return remote(send_buf.at[b], peer.at[b], sc.at[b], rc.at[b], e, 1 - c)

    def along_x(b, h, p, slot):
        return remote(mine_buf.at[b, h], from_x.at[p, slot], sx.at[p, slot], rx.at[p, slot], beside, c)

    def along_y(b, h, p, slot):
        return remote(mine_buf.at[b, h], from_y.at[p, slot], sy.at[p, slot], ry.at[p, slot], above, c)

    def along_z(p, h, up_way):
        b = index(p, y, x)
        d = 0 if up_way else 1
        to = e + 4 if up_way else e - 4
        return remote(mine_buf.at[b, h], from_z.at[p, d, h], sz.at[p, d, h], rz.at[p, d, h], to, c)

    own_at = c * features
    other_at = (1 - c) * features

    def add(b, h, *terms):
        total = mine_buf[b, h].astype(jnp.float32)
        for term in terms:
            total = total + term.astype(jnp.float32)
        mine_buf[b, h] = total.astype(jnp.bfloat16)

    def compute(p):
        count = 4 * capacity
        at = pl.ds(pl.multiple_of(p * count, count), count)

        for l in range(per_group):
            @pl.loop(0, model // width)
            def _(n):
                cut = pl.ds(pl.multiple_of(n * width, width), width)
                got = dot_nt(hid[l, at, :hidden], gate[l, cut])
                got = got + dot_nt(hid[l, at, hidden:], up[l, cut])
                got = got.astype(jnp.bfloat16)
                for q in range(4):
                    partial[q, l * capacity : (l + 1) * capacity, cut] = got[q * capacity : (q + 1) * capacity]

        def back(q, start, store):
            b = p * 4 + q
            slots = slot_ref[b]
            pick = jnp.concatenate([one_hot(slots[l : l + 1], capacity) for l in range(per_group)], axis=0)
            pick = pick.astype(jnp.bfloat16)
            step = 256
            for n in range(features // step):
                cut = pl.ds(pl.multiple_of(start + n * step, 128), step)
                got = lax.dot_general(pick, partial[q, :, cut], TN, preferred_element_type=jnp.float32)
                store(b, n, step, got)

        def store_send(b, n, step, got):
            got = got.astype(jnp.bfloat16)
            for h in range(2):
                send_buf[b, h, :, n * step : (n + 1) * step] = got[h * half : (h + 1) * half]

        def store_mine(b, n, step, got):
            got = got.astype(jnp.bfloat16)
            for h in range(2):
                mine_buf[b, h, :, n * step : (n + 1) * step] = got[h * half : (h + 1) * half]

        @pl.loop(0, 4)
        def _(q):
            back(q, other_at, store_send)
            cross(p * 4 + q).start()

        @pl.loop(0, 4)
        def _(q):
            back(q, own_at, store_mine)

        @pl.loop(0, 4)
        def _(q):
            b = p * 4 + q
            cross(b).wait_recv()
            for h in range(2):
                add(b, h, peer[b, h])

    def relay(p):
        side, over = index(p, y, 1 - x), index(p, 1 - y, x)
        along_x(side, 0, p, 0).wait_recv()
        add(over, 0, from_x[p, 0])
        along_y(over, 0, p, 1).start()
        along_y(over, 1, p, 0).wait_recv()
        add(side, 1, from_y[p, 0])
        along_x(side, 1, p, 2).start()

    def plane_send(p):
        side, over = index(p, y, 1 - x), index(p, 1 - y, x)
        corner = index(p, 1 - y, 1 - x)
        along_x(corner, 0, p, 0).start()
        along_y(corner, 1, p, 0).start()
        along_x(side, 0, p, 1).start()
        along_y(over, 1, p, 2).start()

    def gather(p):
        b = index(p, y, x)
        along_x(b, 0, p, 1).wait_recv()
        along_y(b, 0, p, 1).wait_recv()
        add(b, 0, from_x[p, 1], from_y[p, 1])
        along_x(b, 1, p, 2).wait_recv()
        along_y(b, 1, p, 2).wait_recv()
        add(b, 1, from_x[p, 2], from_y[p, 2])

        @pl.when((p > z) & (z == 0))
        def _():
            for h in range(2):
                along_z(p, h, True).start()

        @pl.when((p < z) & (z == nz - 1))
        def _():
            for h in range(2):
                along_z(p, h, False).start()

    def forward(p):
        b = index(p, y, x)

        @pl.when((p > z) & (z > 0))
        def _():
            for h in range(2):
                along_z(p, h, True).wait_recv()
                add(b, h, from_z[p, 0, h])
                along_z(p, h, True).start()

        @pl.when((p < z) & (z < nz - 1))
        def _():
            for h in range(2):
                along_z(p, h, False).wait_recv()
                add(b, h, from_z[p, 1, h])
                along_z(p, h, False).start()

    def tile(i):
        to = lax.rem(e + i, groups)
        return remote(part_sum.at[to], part_out.at[e], sw.at[i], rw.at[i], to, c)

    @pl.loop(0, nz + 1)
    def _(k):
        @pl.when(k == 0)
        def _():
            for copy in loads:
                copy.wait()

        @pl.when(k < nz)
        def _():
            compute(order(k))

        @pl.when(k == 0)
        def _():
            part_copy.wait_recv()
            part_sum[...] = part_ref[...] + part_peer[...]
            part_out[e] = part_sum[e]

            @pl.loop(1, groups)
            def _(i):
                tile(i).start()

        @pl.when(k >= 1)
        def _():
            relay(order(k - 1))

        @pl.when(k < nz)
        def _():
            plane_send(order(k))

        @pl.when(k >= 1)
        def _():
            gather(order(k - 1))

        @pl.when((k >= 2) & (k < nz))
        def _():
            forward(order(k - 2))

        @pl.when((k == nz - 1) & (k >= 1))
        def _():
            forward(order(k - 1))

    mine = index(z, y, x)
    out_ref[...] = mine_buf[mine]

    @pl.when(z > 0)
    def _():
        for h in range(2):
            along_z(z, h, True).wait_recv()
            out_ref[h] = (out_ref[h].astype(jnp.float32) + from_z[z, 0, h].astype(jnp.float32)).astype(jnp.bfloat16)

    @pl.when(z < nz - 1)
    def _():
        for h in range(2):
            along_z(z, h, False).wait_recv()
            out_ref[h] = (out_ref[h].astype(jnp.float32) + from_z[z, 1, h].astype(jnp.float32)).astype(jnp.bfloat16)

    @pl.loop(1, groups)
    def _(i):
        tile(i).wait()

    part_copy.wait_send()

    @pl.loop(0, nz)
    def _(p):
        for slot in range(3):
            along_x(e, 0, p, slot).wait_send()
            along_y(e, 0, p, slot).wait_send()

        @pl.when((p > z) & (z < nz - 1))
        def _():
            for h in range(2):
                along_z(p, h, True).wait_send()

        @pl.when((p < z) & (z > 0))
        def _():
            for h in range(2):
                along_z(p, h, False).wait_send()

    @pl.loop(0, groups)
    def _(b):
        cross(b).wait_send()


def with_kernels(
    grad_out, combine, expert_ids, saved_gate, saved_up, gate_weight, up_weight, down_weight
):
    groups = lax.axis_size("expert")
    nz = groups // 4
    per_group, model, hidden = gate_weight.shape
    tokens, features = grad_out.shape
    capacity = saved_gate.shape[0] // groups
    experts = groups * per_group
    half = tokens // 2
    slots = groups * capacity
    chosen = expert_ids[:, :, None] == jnp.arange(experts, dtype=jnp.int32)[None, None, :]
    weights = jnp.sum(jnp.where(chosen, combine[:, :, None].astype(jnp.float32), 0.0), axis=1)
    weights = weights.reshape(tokens, groups, per_group).transpose(1, 2, 0)
    weights = jnp.pad(weights, ((0, 0), (0, ROWS - per_group), (0, 0)))
    gate_value = saved_gate.transpose(1, 0, 2)
    up_value = saved_up.transpose(1, 0, 2)
    vmem = pl.BlockSpec(memory_space=pltpu.VMEM)
    hbm = pl.BlockSpec(memory_space=pltpu.HBM)
    bf16, f32 = jnp.bfloat16, jnp.float32
    dma = pltpu.SemaphoreType.DMA
    hid, slot, part = pl.pallas_call(
        functools.partial(dispatch_kernel, nz, capacity),
        name="dispatch",
        out_shape=(
            jax.ShapeDtypeStruct((per_group, slots, 2 * hidden), bf16),
            jax.ShapeDtypeStruct((groups, ROWS, tokens), f32),
            jax.ShapeDtypeStruct((groups, ROWS, tokens), f32),
        ),
        in_specs=[hbm, vmem, hbm, vmem, vmem],
        out_specs=(vmem, vmem, vmem),
        scratch_shapes=[
            pltpu.VMEM((groups, 2, half, features), bf16),
            pltpu.VMEM((groups, 2, half, features), bf16),
            pltpu.VMEM((groups, ROWS, tokens), f32),
            pltpu.VMEM((per_group, hidden, model), bf16),
            pltpu.VMEM((per_group, 4 * capacity, features), bf16),
            pltpu.VMEM((per_group, 4 * capacity, features), bf16),
            pltpu.VMEM((per_group, 4 * capacity, 128), f32),
            dma((2,)),
            dma((nz, 3)), dma((nz, 3)), dma((nz, 3)), dma((nz, 3)),
            dma((nz, 2)), dma((nz, 2)), dma((nz, 2)),
            dma((groups,)), dma((groups,)), dma((groups,)), dma((groups,)),
        ],
        compiler_params=pltpu.CompilerParams(
            collective_id=0, has_side_effects=True, vmem_limit_bytes=VMEM_LIMIT
        ),
    )(grad_out.reshape(2, half, features), weights, down_weight, gate_value, up_value)
    grad_tokens, parts = pl.pallas_call(
        functools.partial(combine_kernel, nz, capacity),
        name="combine",
        out_shape=(
            jax.ShapeDtypeStruct((2, half, features), bf16),
            jax.ShapeDtypeStruct((groups, ROWS, tokens), f32),
        ),
        in_specs=[hbm, vmem, vmem, hbm, hbm],
        out_specs=(vmem, vmem),
        scratch_shapes=[
            pltpu.VMEM((per_group, slots, 2 * hidden), bf16),
            pltpu.VMEM((per_group, model, hidden), bf16),
            pltpu.VMEM((per_group, model, hidden), bf16),
            pltpu.VMEM((4, per_group * capacity, model), bf16),
            pltpu.VMEM((groups, 2, half, features), bf16),
            pltpu.VMEM((groups, 2, half, features), bf16),
            pltpu.VMEM((groups, 2, half, features), bf16),
            pltpu.VMEM((nz, 3, half, features), bf16),
            pltpu.VMEM((nz, 3, half, features), bf16),
            pltpu.VMEM((nz, 2, 2, half, features), bf16),
            pltpu.VMEM((groups, ROWS, tokens), f32),
            pltpu.VMEM((groups, ROWS, tokens), f32),
            dma((per_group, 3)),
            dma((nz, 3)), dma((nz, 3)), dma((nz, 3)), dma((nz, 3)),
            dma((nz, 2, 2)), dma((nz, 2, 2)),
            dma((groups,)), dma((groups,)), dma((groups,)), dma((groups,)),
            dma(()), dma(()),
        ],
        compiler_params=pltpu.CompilerParams(
            collective_id=1, has_side_effects=True, vmem_limit_bytes=VMEM_LIMIT
        ),
    )(hid, slot, part, gate_weight, up_weight)
    parts = parts[:, :per_group].transpose(2, 0, 1).reshape(tokens, 1, experts)
    grad_combine = jnp.sum(jnp.where(chosen, parts, 0.0), axis=2).astype(jnp.bfloat16)
    return grad_tokens.reshape(tokens, features), grad_combine


def with_collectives(
    grad_out, combine, expert_ids, saved_gate, saved_up, gate_weight, up_weight, down_weight
):
    groups = lax.axis_size("expert")
    per_group = gate_weight.shape[0]
    tokens = grad_out.shape[0]
    capacity = saved_gate.shape[0] // groups
    hidden = saved_gate.shape[2]
    experts = groups * per_group
    chosen = expert_ids[:, :, None] == jnp.arange(experts, dtype=jnp.int32)[None, None, :]
    weights = jnp.sum(jnp.where(chosen, combine[:, :, None].astype(jnp.float32), 0.0), axis=1)
    weights = weights.astype(jnp.bfloat16).reshape(tokens, groups, per_group)
    weights = lax.all_to_all(
        weights.transpose(1, 2, 0), "expert", split_axis=0, concat_axis=0, tiled=True
    )
    rows = lax.all_gather(grad_out, "expert", axis=0, tiled=True)
    rows = lax.all_gather(rows, "etp", axis=1, tiled=True)
    rows = rows.reshape(groups, tokens, -1)
    named = (weights > 0).astype(jnp.float32)
    position = jnp.cumsum(named, axis=2) - named
    slot = jnp.where(named > 0, position, -1.0)
    select = slot[:, :, None, :] == jnp.arange(capacity, dtype=jnp.float32)[None, None, :, None]
    scale = jnp.sum(jnp.where(select, weights[:, :, None, :].astype(jnp.float32), 0.0), axis=3)
    scale = scale.transpose(1, 0, 2)[..., None]
    select = select.astype(jnp.bfloat16)
    slot_rows = jnp.einsum(
        "blct,btd->lbcd", select, rows, preferred_element_type=jnp.bfloat16
    )
    grad_hidden = jnp.einsum(
        "lbcd,lfd->lbcf", slot_rows, down_weight, preferred_element_type=jnp.float32
    )
    gate_value = saved_gate.reshape(groups, capacity, per_group, hidden).transpose(2, 0, 1, 3)
    up_value = saved_up.reshape(groups, capacity, per_group, hidden).transpose(2, 0, 1, 3)
    gate_value = gate_value.astype(jnp.float32)
    up_value = up_value.astype(jnp.float32)
    gate_sigmoid = jax.nn.sigmoid(gate_value)
    activated = gate_value * gate_sigmoid
    weight_part = jnp.sum(grad_hidden * activated * up_value, axis=3)
    scaled = scale * grad_hidden
    grad_gate = (
        scaled * up_value * gate_sigmoid * (1.0 + gate_value * (1.0 - gate_sigmoid))
    ).astype(jnp.bfloat16)
    grad_up = (scaled * activated).astype(jnp.bfloat16)
    weight_tok = jnp.einsum(
        "blct,lbc->blt", select, weight_part.astype(jnp.bfloat16),
        preferred_element_type=jnp.float32,
    ).astype(jnp.bfloat16)
    weight_tok = lax.psum(weight_tok, "etp")
    weight_tok = lax.all_to_all(weight_tok, "expert", split_axis=0, concat_axis=0, tiled=True)
    weight_tok = weight_tok.transpose(2, 0, 1).reshape(tokens, 1, experts)
    grad_combine = jnp.sum(
        jnp.where(chosen, weight_tok.astype(jnp.float32), 0.0), axis=2
    ).astype(jnp.bfloat16)
    partial = jnp.einsum(
        "lbcf,ldf->lbcd", grad_gate, gate_weight, preferred_element_type=jnp.float32
    )
    partial = partial + jnp.einsum(
        "lbcf,ldf->lbcd", grad_up, up_weight, preferred_element_type=jnp.float32
    )
    partial = jnp.einsum(
        "blct,lbcd->btd", select, partial.astype(jnp.bfloat16),
        preferred_element_type=jnp.float32,
    ).astype(jnp.bfloat16)
    partial = partial.reshape(groups * tokens, -1)
    partial = lax.psum_scatter(partial, "etp", scatter_dimension=1, tiled=True)
    grad_tokens = lax.psum_scatter(partial, "expert", scatter_dimension=0, tiled=True)
    return (grad_tokens, grad_combine)


def on_device(grad_out, *rest):
    groups = lax.axis_size("expert")
    held = 4 * groups * grad_out.size
    if groups % 4 == 0 and lax.axis_size("etp") == 2 and held <= TOKEN_BYTES:
        return with_kernels(grad_out, *rest)
    return with_collectives(grad_out, *rest)


def solution(mesh):
    in_specs = (
        P("expert", "etp"),
        P("expert", None),
        P("expert", None),
        P(None, "expert", "etp"),
        P(None, "expert", "etp"),
        P("expert", None, "etp"),
        P("expert", None, "etp"),
        P("expert", "etp", None),
    )
    out_specs = (P("expert", "etp"), P("expert", None))
    return jax.shard_map(
        on_device, mesh=mesh, in_specs=in_specs, out_specs=out_specs, check_vma=False
    )
```

```python
import functools

import jax
import jax.numpy as jnp
from jax import lax
from jax.experimental import pallas as pl
from jax.experimental.pallas import tpu as pltpu
from jax.sharding import PartitionSpec as P

MESH = pl.DeviceIdType.MESH
VMEM_LIMIT = 67_043_328
TOKEN_BYTES = 24 * 2**20
NT = (((1,), (1,)), ((), ()))
TN = (((0,), (0,)), ((), ()))
ROWS = 8


def dot_nt(a, b):
    return lax.dot_general(a, b, NT, preferred_element_type=jnp.float32)


def place():
    e = lax.axis_index("expert")
    c = lax.axis_index("etp")
    return e, c, e // 4, (e // 2) % 2, e % 2


def index(z, y, x):
    return z * 4 + y * 2 + x


def enter(groups, e, c):
    barrier = pltpu.get_barrier_semaphore()

    @pl.loop(1, groups)
    def _(i):
        pl.semaphore_signal(
            barrier, inc=1, device_id=(lax.rem(e + i, groups), c), device_id_type=MESH
        )

    pl.semaphore_signal(barrier, inc=1, device_id=(e, 1 - c), device_id_type=MESH)
    pl.semaphore_wait(barrier, groups)


def remote(src, dst, send, recv, expert, core):
    return pltpu.make_async_remote_copy(
        src_ref=src,
        dst_ref=dst,
        send_sem=send,
        recv_sem=recv,
        device_id=(expert, core),
        device_id_type=MESH,
    )


def one_hot(slot_row, capacity):
    tokens = slot_row.shape[1]
    at = lax.broadcasted_iota(jnp.int32, (capacity, tokens), 0).astype(jnp.float32)
    return jnp.where(slot_row == at, 1.0, 0.0)


def fused_kernel(
    nz, capacity, ra, rr,
    x_hbm, weights_ref, down_hbm, gate_hbm, up_hbm, saved_gate_hbm, saved_up_hbm,
    out_ref, part_out,
    own, other, mine, send, weights, slots_at, part, part_peer, part_sum,
    down, gate, up, work, hid, scale, saved_gate, saved_up, from_x, from_y, from_zc, from_zr,
    load_sem, saved_sem,
    asx, arx, asy, ary, asu, asd, arz, aru, ard, arr, acs, acr, sw, rw,
    rsx, rrx, rsy, rry, zcs, zcr, zrs, zrr, bcs, bcr, sp, rp, qs, qr, credit,
):
    e, c, z, y, x = place()
    groups = nz * 4
    per_group, hidden, model = down.shape
    tokens = weights.shape[2]
    half, features = own.shape[2:]
    width = 256
    pieces = hidden // width
    count = 4 * capacity
    beside, above = index(z, y, 1 - x), index(z, 1 - y, x)
    whole = pl.ds(0, half)
    tail = pl.ds(ra, half - ra)

    load_x = pltpu.make_async_copy(x_hbm, own.at[e], load_sem.at[0])
    load_x.start()
    loads = [
        pltpu.make_async_copy(src, dst, load_sem.at[i + 1])
        for i, (src, dst) in enumerate(((down_hbm, down), (gate_hbm, gate), (up_hbm, up)))
    ]

    def order(k):
        low = jnp.where(k <= z, z - k, k)
        back = nz - 1 - z
        high = jnp.where(k <= back, z + k, nz - 1 - k)
        return jnp.where(z < nz // 2, low, high)

    def passing(i):
        low = jnp.where(i < nz - 1 - z, z + 1 + i, nz - 2 - i)
        high = jnp.where(i < z, z - 1 - i, i + 1)
        return jnp.where(z < nz // 2, low, high)

    def load_saved(p):
        at = pl.ds(pl.multiple_of(p * count, count), count)
        return [
            pltpu.make_async_copy(saved_gate_hbm.at[:, at], saved_gate, saved_sem.at[0]),
            pltpu.make_async_copy(saved_up_hbm.at[:, at], saved_up, saved_sem.at[1]),
        ]

    weights[e] = weights_ref[e]
    enter(groups, e, c)

    def a_x(b, h, p, slot, rows):
        at = own.at[b, h, rows]
        return remote(at, at, asx.at[p, slot], arx.at[p, slot], beside, c)

    def a_y(b, h, p, slot, rows):
        at = own.at[b, h, rows]
        return remote(at, at, asy.at[p, slot], ary.at[p, slot], above, c)

    def a_z(p, h, up_way):
        at = own.at[index(p, y, x), h]
        sems = asu if up_way else asd
        return remote(at, at, sems.at[p, h], arz.at[p, h], e + 4 if up_way else e - 4, c)

    def others(p):
        return index(p, y, 1 - x), index(p, 1 - y, x), index(p, 1 - y, 1 - x)

    def a_r(p, j, up_way):
        at = own.at[others(p)[j], :, pl.ds(0, ra)]
        sems = aru if up_way else ard
        return remote(at, at, sems.at[p, j], arr.at[p, j], e + 4 if up_way else e - 4, c)

    def cross(b):
        return remote(own.at[b], other.at[b], acs.at[b], acr.at[b], e, 1 - c)

    def a_send(p, rows):
        b = index(p, y, x)
        a_x(b, 0, p, 0, rows).start()
        a_y(b, 1, p, 1, rows).start()
        a_x(b, 1, p, 1, rows).start()
        a_y(b, 0, p, 0, rows).start()

    def a_relay(p, rows):
        side, over, _ = others(p)
        a_x(side, 0, p, 0, rows).wait_recv()
        a_y(side, 0, p, 2, rows).start()
        a_y(over, 1, p, 1, rows).wait_recv()
        a_x(over, 1, p, 2, rows).start()

    def a_arrive(far):
        @pl.when(z - far >= 0)
        def _():
            for h in range(2):
                a_z(z - far, h, True).wait_recv()

                @pl.when(z < nz - 1)
                def _():
                    a_z(z - far, h, True).start()

        @pl.when(z + far < nz)
        def _():
            for h in range(2):
                a_z(z + far, h, False).wait_recv()

                @pl.when(z > 0)
                def _():
                    a_z(z + far, h, False).start()

        @pl.when(far < nz)
        def _():
            after = order(far)
            a_send(after, tail)
            cross(index(after, y, x)).start()

    def a_spread(j):
        @pl.when(z < nz - 1)
        def _():
            a_r(z, j, True).start()

        @pl.when(z > 0)
        def _():
            a_r(z, j, False).start()

    def a_finish_own():
        side, over, corner = others(z)
        a_x(side, 1, z, 1, whole).wait_recv()
        a_spread(0)
        cross(side).start()
        a_y(over, 0, z, 0, whole).wait_recv()
        a_spread(1)
        cross(over).start()
        a_y(corner, 0, z, 2, whole).wait_recv()
        a_x(corner, 1, z, 2, whole).wait_recv()
        a_spread(2)
        cross(corner).start()

    def a_finish(k, p):
        @pl.when(z - k >= 0)
        def _():
            for j in range(3):
                a_r(z - k, j, True).wait_recv()

                @pl.when(z < nz - 1)
                def _():
                    a_r(z - k, j, True).start()

        @pl.when(z + k < nz)
        def _():
            for j in range(3):
                a_r(z + k, j, False).wait_recv()

                @pl.when(z > 0)
                def _():
                    a_r(z + k, j, False).start()

        side, over, corner = others(p)
        a_x(side, 1, p, 1, tail).wait_recv()
        cross(side).start()
        a_y(over, 0, p, 0, tail).wait_recv()
        cross(over).start()
        a_y(corner, 0, p, 2, tail).wait_recv()
        a_x(corner, 1, p, 2, tail).wait_recv()
        cross(corner).start()

    def tile(i):
        to = lax.rem(e + i, groups)
        return remote(weights_ref.at[to], weights.at[e], sw.at[i], rw.at[i], to, c)

    own_at = c * features
    other_at = (1 - c) * features

    def apart(first, second):
        none = jnp.zeros_like(first)
        upper = jnp.concatenate([first, none], axis=1)
        lower = jnp.concatenate([none, second], axis=1)
        return jnp.concatenate([upper, lower], axis=0).astype(jnp.bfloat16)

    def picks_of(b):
        slots = slots_at[b]
        return [one_hot(slots[l : l + 1], capacity) for l in range(per_group)]

    def gather(p, i):
        both = []
        for j in range(2):
            b, q = p * 4 + 2 * i + j, 2 * i + j
            table = weights[b]
            picks = picks_of(b)
            for l in range(per_group):
                amount = jnp.sum(picks[l] * table[l : l + 1], axis=1, keepdims=True)
                scale[l, pl.ds(q * capacity, capacity)] = jnp.broadcast_to(amount, (capacity, 128))
            both.append(jnp.concatenate(picks, axis=0))
        pick = apart(*both)
        for s, held in ((0, own), (1, other)):
            block = held[pl.ds(p * 4 + 2 * i, 2)].reshape(2 * tokens, features)
            got = jnp.dot(pick, block, preferred_element_type=jnp.float32).astype(jnp.bfloat16)
            for j in range(2):
                for l in range(per_group):
                    at = (j * per_group + l) * capacity
                    to = l * count + (2 * i + j) * capacity
                    work[s, pl.ds(to, capacity)] = got[at : at + capacity]

    def hidden_grads(p, l):
        weight_part = jnp.zeros((count, 1), jnp.float32)
        at = pl.ds(pl.multiple_of(l * count, count), count)
        for j in range(pieces):
            cut = slice(j * width, (j + 1) * width)
            grad = dot_nt(work[0, at], down[l, cut, pl.ds(pl.multiple_of(own_at, 128), features)])
            grad = grad + dot_nt(work[1, at], down[l, cut, pl.ds(pl.multiple_of(other_at, 128), features)])
            gate_value = saved_gate[l, :, cut].astype(jnp.float32)
            up_value = saved_up[l, :, cut].astype(jnp.float32)
            sigmoid = jax.nn.sigmoid(gate_value)
            active = gate_value * sigmoid
            weight_part = weight_part + jnp.sum(grad * active * up_value, axis=1, keepdims=True)
            scaled = scale[l][:, :1] * grad
            grad_gate = scaled * up_value * sigmoid * (1.0 + gate_value * (1.0 - sigmoid))
            hid[l, :, cut] = grad_gate.astype(jnp.bfloat16)
            cut = slice(hidden + j * width, hidden + (j + 1) * width)
            hid[l, :, cut] = (scaled * active).astype(jnp.bfloat16)
        weight_part = weight_part.astype(jnp.bfloat16).astype(jnp.float32)
        for q in range(4):
            b = p * 4 + q
            pick = one_hot(slots_at[b, pl.ds(l, 1)], capacity)
            piece = weight_part[q * capacity : (q + 1) * capacity]
            part[b, pl.ds(l, 1)] = jnp.sum(pick * piece, axis=0, keepdims=True)

    def back_cross(p, q):
        return remote(send.at[q], other.at[p * 4 + q], bcs.at[q], bcr.at[q], e, 1 - c)

    def front(p):
        @pl.loop(0, 4)
        def _(q):
            cross(p * 4 + q).wait_recv()

        @pl.loop(0, 2)
        def _(i):
            gather(p, i)

        pl.semaphore_signal(credit, inc=1, device_id=(e, 1 - c), device_id_type=MESH)
        for copy in load_saved(p):
            copy.wait()

        @pl.loop(0, per_group)
        def _(l):
            hidden_grads(p, l)

    def products(s, start):
        @pl.loop(0, per_group)
        def _(l):
            rows = pl.ds(pl.multiple_of(start, 128), features)
            got = dot_nt(hid[l, :, :hidden], gate[l, rows])
            got = got + dot_nt(hid[l, :, hidden:], up[l, rows])
            got = got.astype(jnp.bfloat16)
            for q in range(4):
                at = q * per_group * capacity + l * capacity
                work[s, pl.ds(at, capacity)] = got[q * capacity : (q + 1) * capacity]

    def to_tokens(p, i, s):
        pick = apart(*[jnp.concatenate(picks_of(p * 4 + 2 * i + j), axis=0) for j in range(2)])
        size = 2 * per_group * capacity
        rows = pl.ds(pl.multiple_of(i * size, size), size)
        got = lax.dot_general(pick, work[s, rows], TN, preferred_element_type=jnp.float32)
        return got.astype(jnp.bfloat16).reshape(2, 2, half, features)

    def back(k, p):
        products(1, other_at)
        pl.semaphore_wait(credit, 1)

        @pl.loop(0, 2)
        def _(i):
            for j in range(2):
                @pl.when(k > 0)
                def _():
                    back_cross(p, 2 * i + j).wait_send()

            send[pl.ds(2 * i, 2)] = to_tokens(p, i, 1)
            for j in range(2):
                back_cross(p, 2 * i + j).start()

        products(0, own_at)

        @pl.loop(0, 2)
        def _(i):
            got = to_tokens(p, i, 0)
            for j in range(2):
                b = p * 4 + 2 * i + j
                back_cross(p, 2 * i + j).wait_recv()
                mine[b] = (got[j].astype(jnp.float32) + other[b].astype(jnp.float32)).astype(jnp.bfloat16)

    low = pl.ds(0, rr)
    high = pl.ds(rr, half - rr)

    def add(b, h, rows, *terms):
        total = mine[b, h, rows].astype(jnp.float32)
        for term in terms:
            total = total + term.astype(jnp.float32)
        mine[b, h, rows] = total.astype(jnp.bfloat16)

    def r_x(b, h, t, slot, rows):
        dst = from_x.at[t, slot, pl.ds(0, rows.size)]
        return remote(mine.at[b, h, rows], dst, rsx.at[t, slot], rrx.at[t, slot], beside, c)

    def r_y(b, h, t, slot, rows):
        dst = from_y.at[t, slot, pl.ds(0, rows.size)]
        return remote(mine.at[b, h, rows], dst, rsy.at[t, slot], rry.at[t, slot], above, c)

    def landing(p, up_way):
        return p if up_way else jnp.where(p == z - 1, nz, p)

    def r_zc(p, h, up_way):
        t = landing(p, up_way)
        src = mine.at[index(p, y, x), h, high]
        return remote(src, from_zc.at[t, h], zcs.at[p, h], zcr.at[t, h], e + 4 if up_way else e - 4, c)

    def r_zr(p, q, up_way):
        t = landing(p, up_way)
        src = mine.at[p * 4 + q, :, low]
        return remote(src, from_zr.at[t, q], zrs.at[p, q], zrr.at[t, q], e + 4 if up_way else e - 4, c)

    def got_zc(t, h):
        return remote(mine.at[e, h, high], from_zc.at[t, h], zcs.at[0, h], zcr.at[t, h], e, 1 - c)

    def got_zr(t, q):
        return remote(mine.at[q, :, low], from_zr.at[t, q], zrs.at[0, q], zrr.at[t, q], e, 1 - c)

    def r_send(p, t, rows):
        side, over, corner = others(p)
        r_x(corner, 0, t, 0, rows).start()
        r_y(corner, 1, t, 0, rows).start()
        r_x(side, 0, t, 1, rows).start()
        r_y(over, 1, t, 2, rows).start()

    def r_relay(p, t, rows):
        side, over, _ = others(p)
        n = pl.ds(0, rows.size)
        r_x(side, 0, t, 0, rows).wait_recv()
        add(over, 0, rows, from_x[t, 0, n])
        r_y(over, 0, t, 1, rows).start()
        r_y(over, 1, t, 0, rows).wait_recv()
        add(side, 1, rows, from_y[t, 0, n])
        r_x(side, 1, t, 2, rows).start()

    def r_gather(p, t, rows):
        b = index(p, y, x)
        n = pl.ds(0, rows.size)
        for h in range(2):
            r_x(b, h, t, h + 1, rows).wait_recv()
            r_y(b, h, t, h + 1, rows).wait_recv()
            add(b, h, rows, from_x[t, h + 1, n], from_y[t, h + 1, n])

    def col_start(p):
        @pl.when((p > z) & (z == 0))
        def _():
            for h in range(2):
                r_zc(p, h, True).start()

        @pl.when((p < z) & (z == nz - 1))
        def _():
            for h in range(2):
                r_zc(p, h, False).start()

    def col_pass(p):
        b = index(p, y, x)

        def go(up_way):
            for h in range(2):
                got_zc(p, h).wait_recv()
                add(b, h, high, from_zc[p, h])
                r_zc(p, h, up_way).start()

        @pl.when((p > z) & (z > 0))
        def _():
            go(True)

        @pl.when((p < z) & (z < nz - 1))
        def _():
            go(False)

    def rows_start(p):
        @pl.when((p > z) & (z == 0))
        def _():
            for q in range(4):
                r_zr(p, q, True).start()

        @pl.when((p < z) & (z == nz - 1))
        def _():
            for q in range(4):
                r_zr(p, q, False).start()

    def rows_add(t, q, b):
        got_zr(t, q).wait_recv()
        for h in range(2):
            add(b, h, low, from_zr[t, q, h])

    def rows_pass(p):
        def go(up_way):
            @pl.loop(0, 4)
            def _(q):
                rows_add(p, q, p * 4 + q)
                r_zr(p, q, up_way).start()

        @pl.when((p > z) & (z > 0))
        def _():
            go(True)

        @pl.when((p < z) & (z < nz - 1))
        def _():
            go(False)

    def rows_final():
        @pl.when(z > 0)
        def _():
            @pl.loop(0, 4)
            def _(q):
                rows_add(z, q, z * 4 + q)

        @pl.when(z < nz - 1)
        def _():
            @pl.loop(0, 4)
            def _(q):
                rows_add(nz, q, z * 4 + q)

    @pl.loop(1, groups)
    def _(i):
        tile(i).start()

    load_x.wait()
    a_send(z, whole)
    for h in range(2):
        @pl.when(z < nz - 1)
        def _():
            a_z(z, h, True).start()

        @pl.when(z > 0)
        def _():
            a_z(z, h, False).start()

    cross(e).start()
    for copy in load_saved(z):
        copy.start()
    for copy in loads:
        copy.start()
    part[...] = jnp.zeros_like(part)
    a_relay(z, whole)
    a_arrive(1)

    @pl.loop(1, groups)
    def _(i):
        tile(i).wait_recv()

    named = (weights[...] > 0).astype(jnp.bfloat16).reshape(groups * ROWS, tokens)
    first = lax.broadcasted_iota(jnp.int32, (tokens, tokens), 0)
    second = lax.broadcasted_iota(jnp.int32, (tokens, tokens), 1)
    before = (first < second).astype(jnp.bfloat16)
    position = jnp.dot(named, before, preferred_element_type=jnp.float32)
    slots_at[...] = jnp.where(named > 0, position, -1.0).reshape(groups, ROWS, tokens)

    @pl.loop(0, nz)
    def _(k):
        p = order(k)

        @pl.when(k == 0)
        def _():
            a_finish_own()
            for copy in loads:
                copy.wait()

        @pl.when(k > 0)
        def _():
            a_finish(k, p)

        front(p)

        @pl.when(k + 1 < nz)
        def _():
            for copy in load_saved(order(k + 1)):
                copy.start()
            a_relay(order(k + 1), tail)
            a_arrive(k + 2)

        back(k, p)

        @pl.when(k > 0)
        def _():
            rows_start(p)

        @pl.when(k == nz - 2)
        def _():
            @pl.loop(1, nz - 1)
            def _(i):
                r_send(order(i), order(i), high)

    part_copy = remote(part, part_peer, sp, rp, e, 1 - c)
    part_copy.start()

    def part_tile(i):
        to = lax.rem(e + i, groups)
        return remote(part_sum.at[to], part_out.at[e], qs.at[i], qr.at[i], to, c)

    last = order(nz - 1)
    r_send(last, last, high)
    for i in range(1, nz - 1):
        r_relay(order(i), order(i), high)
    rows_pass(passing(0))
    r_relay(last, last, high)
    r_send(z, z, high)
    part_copy.wait()
    part_sum[...] = part[...] + part_peer[...]
    part_out[e] = part_sum[e]

    @pl.loop(1, groups)
    def _(i):
        part_tile(i).start()

    for i in range(1, nz):
        p = order(i)
        r_gather(p, p, high)
        col_start(p)
        if i < nz - 1:
            rows_pass(passing(i))
    rows_final()
    r_send(z, nz, low)
    r_relay(z, z, high)
    for i in range(nz - 2):
        col_pass(passing(i))
    r_relay(z, nz, low)
    col_pass(passing(nz - 2))
    r_gather(z, z, high)
    r_gather(z, nz, low)

    at_home = index(z, y, x)
    out_ref[...] = mine[at_home]

    def col_final(t):
        for h in range(2):
            got_zc(t, h).wait_recv()
            total = out_ref[h, high].astype(jnp.float32) + from_zc[t, h].astype(jnp.float32)
            out_ref[h, high] = total.astype(jnp.bfloat16)

    @pl.when(z > 0)
    def _():
        col_final(z)

    @pl.when(z < nz - 1)
    def _():
        col_final(nz)

    @pl.loop(1, groups)
    def _(i):
        tile(i).wait_send()
        part_tile(i).wait()

    def sent_xy(p, rows):
        for slot in range(3):
            a_x(e, 0, p, slot, rows).wait_send()
            a_y(e, 0, p, slot, rows).wait_send()

    sent_xy(z, whole)
    for slot in range(3):
        r_x(e, 0, nz, slot, low).wait_send()
        r_y(e, 0, nz, slot, low).wait_send()

    @pl.loop(0, nz)
    def _(p):
        @pl.when(p != z)
        def _():
            sent_xy(p, tail)

        for slot in range(3):
            r_x(e, 0, p, slot, high).wait_send()
            r_y(e, 0, p, slot, high).wait_send()

        @pl.when((p <= z) & (z < nz - 1))
        def _():
            for h in range(2):
                a_z(p, h, True).wait_send()
            for j in range(3):
                a_r(p, j, True).wait_send()

        @pl.when((p >= z) & (z > 0))
        def _():
            for h in range(2):
                a_z(p, h, False).wait_send()
            for j in range(3):
                a_r(p, j, False).wait_send()

        @pl.when((p > z) & (z < nz - 1))
        def _():
            for h in range(2):
                r_zc(p, h, True).wait_send()
            for q in range(4):
                r_zr(p, q, True).wait_send()

        @pl.when((p < z) & (z > 0))
        def _():
            for h in range(2):
                r_zc(p, h, False).wait_send()
            for q in range(4):
                r_zr(p, q, False).wait_send()

    @pl.loop(0, groups)
    def _(b):
        cross(b).wait_send()

    @pl.loop(0, 4)
    def _(q):
        back_cross(z, q).wait_send()


def with_kernel(
    grad_out, combine, expert_ids, saved_gate, saved_up, gate_weight, up_weight, down_weight
):
    groups = lax.axis_size("expert")
    nz = groups // 4
    per_group, model, hidden = gate_weight.shape
    tokens, features = grad_out.shape
    capacity = saved_gate.shape[0] // groups
    experts = groups * per_group
    half = tokens // 2
    ra = half // 64 * 16
    rr = half // 64 * 16
    chosen = expert_ids[:, :, None] == jnp.arange(experts, dtype=jnp.int32)[None, None, :]
    weights = jnp.sum(jnp.where(chosen, combine[:, :, None].astype(jnp.float32), 0.0), axis=1)
    weights = weights.reshape(tokens, groups, per_group).transpose(1, 2, 0)
    weights = jnp.pad(weights, ((0, 0), (0, ROWS - per_group), (0, 0)))
    gate_value = saved_gate.transpose(1, 0, 2)
    up_value = saved_up.transpose(1, 0, 2)
    vmem = pl.BlockSpec(memory_space=pltpu.VMEM)
    hbm = pl.BlockSpec(memory_space=pltpu.HBM)
    bf16, f32 = jnp.bfloat16, jnp.float32
    dma = pltpu.SemaphoreType.DMA
    table = pltpu.VMEM((groups, ROWS, tokens), f32)
    blocks = pltpu.VMEM((groups, 2, half, features), bf16)
    count = 4 * capacity
    grad_tokens, parts = pl.pallas_call(
        functools.partial(fused_kernel, nz, capacity, ra, rr),
        name="experts",
        out_shape=(
            jax.ShapeDtypeStruct((2, half, features), bf16),
            jax.ShapeDtypeStruct((groups, ROWS, tokens), f32),
        ),
        in_specs=[hbm, vmem, hbm, hbm, hbm, hbm, hbm],
        out_specs=(vmem, vmem),
        scratch_shapes=[
            blocks, blocks, blocks,
            pltpu.VMEM((4, 2, half, features), bf16),
            table, table, table, table, table,
            pltpu.VMEM((per_group, hidden, model), bf16),
            pltpu.VMEM((per_group, model, hidden), bf16),
            pltpu.VMEM((per_group, model, hidden), bf16),
            pltpu.VMEM((2, per_group * count, features), bf16),
            pltpu.VMEM((per_group, count, 2 * hidden), bf16),
            pltpu.VMEM((per_group, count, 128), f32),
            pltpu.VMEM((per_group, count, hidden), bf16),
            pltpu.VMEM((per_group, count, hidden), bf16),
            pltpu.VMEM((nz + 1, 3, half - rr, features), bf16),
            pltpu.VMEM((nz + 1, 3, half - rr, features), bf16),
            pltpu.VMEM((nz + 1, 2, half - rr, features), bf16),
            pltpu.VMEM((nz + 1, 4, 2, rr, features), bf16),
            dma((4,)), dma((2,)),
            dma((nz, 3)), dma((nz, 3)), dma((nz, 3)), dma((nz, 3)),
            dma((nz, 2)), dma((nz, 2)), dma((nz, 2)),
            dma((nz, 3)), dma((nz, 3)), dma((nz, 3)),
            dma((groups,)), dma((groups,)), dma((groups,)), dma((groups,)),
            dma((nz + 1, 3)), dma((nz + 1, 3)), dma((nz + 1, 3)), dma((nz + 1, 3)),
            dma((nz, 2)), dma((nz + 1, 2)), dma((nz, 4)), dma((nz + 1, 4)),
            dma((4,)), dma((4,)), dma(()), dma(()), dma((groups,)), dma((groups,)),
            pltpu.SemaphoreType.REGULAR,
        ],
        compiler_params=pltpu.CompilerParams(
            collective_id=0, has_side_effects=True, vmem_limit_bytes=VMEM_LIMIT
        ),
    )(grad_out.reshape(2, half, features), weights, down_weight, gate_weight, up_weight, gate_value, up_value)
    parts = parts[:, :per_group].transpose(2, 0, 1).reshape(tokens, 1, experts)
    grad_combine = jnp.sum(jnp.where(chosen, parts, 0.0), axis=2).astype(jnp.bfloat16)
    return grad_tokens.reshape(tokens, features), grad_combine


def with_collectives(
    grad_out, combine, expert_ids, saved_gate, saved_up, gate_weight, up_weight, down_weight
):
    groups = lax.axis_size("expert")
    per_group = gate_weight.shape[0]
    tokens = grad_out.shape[0]
    capacity = saved_gate.shape[0] // groups
    hidden = saved_gate.shape[2]
    experts = groups * per_group
    chosen = expert_ids[:, :, None] == jnp.arange(experts, dtype=jnp.int32)[None, None, :]
    weights = jnp.sum(jnp.where(chosen, combine[:, :, None].astype(jnp.float32), 0.0), axis=1)
    weights = weights.astype(jnp.bfloat16).reshape(tokens, groups, per_group)
    weights = lax.all_to_all(
        weights.transpose(1, 2, 0), "expert", split_axis=0, concat_axis=0, tiled=True
    )
    rows = lax.all_gather(grad_out, "expert", axis=0, tiled=True)
    rows = lax.all_gather(rows, "etp", axis=1, tiled=True)
    rows = rows.reshape(groups, tokens, -1)
    named = (weights > 0).astype(jnp.float32)
    position = jnp.cumsum(named, axis=2) - named
    slot = jnp.where(named > 0, position, -1.0)
    select = slot[:, :, None, :] == jnp.arange(capacity, dtype=jnp.float32)[None, None, :, None]
    scale = jnp.sum(jnp.where(select, weights[:, :, None, :].astype(jnp.float32), 0.0), axis=3)
    scale = scale.transpose(1, 0, 2)[..., None]
    select = select.astype(jnp.bfloat16)
    slot_rows = jnp.einsum(
        "blct,btd->lbcd", select, rows, preferred_element_type=jnp.bfloat16
    )
    grad_hidden = jnp.einsum(
        "lbcd,lfd->lbcf", slot_rows, down_weight, preferred_element_type=jnp.float32
    )
    gate_value = saved_gate.reshape(groups, capacity, per_group, hidden).transpose(2, 0, 1, 3)
    up_value = saved_up.reshape(groups, capacity, per_group, hidden).transpose(2, 0, 1, 3)
    gate_value = gate_value.astype(jnp.float32)
    up_value = up_value.astype(jnp.float32)
    gate_sigmoid = jax.nn.sigmoid(gate_value)
    activated = gate_value * gate_sigmoid
    weight_part = jnp.sum(grad_hidden * activated * up_value, axis=3)
    scaled = scale * grad_hidden
    grad_gate = (
        scaled * up_value * gate_sigmoid * (1.0 + gate_value * (1.0 - gate_sigmoid))
    ).astype(jnp.bfloat16)
    grad_up = (scaled * activated).astype(jnp.bfloat16)
    weight_tok = jnp.einsum(
        "blct,lbc->blt", select, weight_part.astype(jnp.bfloat16),
        preferred_element_type=jnp.float32,
    ).astype(jnp.bfloat16)
    weight_tok = lax.psum(weight_tok, "etp")
    weight_tok = lax.all_to_all(weight_tok, "expert", split_axis=0, concat_axis=0, tiled=True)
    weight_tok = weight_tok.transpose(2, 0, 1).reshape(tokens, 1, experts)
    grad_combine = jnp.sum(
        jnp.where(chosen, weight_tok.astype(jnp.float32), 0.0), axis=2
    ).astype(jnp.bfloat16)
    partial = jnp.einsum(
        "lbcf,ldf->lbcd", grad_gate, gate_weight, preferred_element_type=jnp.float32
    )
    partial = partial + jnp.einsum(
        "lbcf,ldf->lbcd", grad_up, up_weight, preferred_element_type=jnp.float32
    )
    partial = jnp.einsum(
        "blct,lbcd->btd", select, partial.astype(jnp.bfloat16),
        preferred_element_type=jnp.float32,
    ).astype(jnp.bfloat16)
    partial = partial.reshape(groups * tokens, -1)
    partial = lax.psum_scatter(partial, "etp", scatter_dimension=1, tiled=True)
    grad_tokens = lax.psum_scatter(partial, "expert", scatter_dimension=0, tiled=True)
    return (grad_tokens, grad_combine)


def on_device(grad_out, *rest):
    groups = lax.axis_size("expert")
    held = 4 * groups * grad_out.size
    if groups % 4 == 0 and lax.axis_size("etp") == 2 and held <= TOKEN_BYTES:
        return with_kernel(grad_out, *rest)
    return with_collectives(grad_out, *rest)


def solution(mesh):
    in_specs = (
        P("expert", "etp"),
        P("expert", None),
        P("expert", None),
        P(None, "expert", "etp"),
        P(None, "expert", "etp"),
        P("expert", None, "etp"),
        P("expert", None, "etp"),
        P("expert", "etp", None),
    )
    out_specs = (P("expert", "etp"), P("expert", None))
    return jax.shard_map(
        on_device, mesh=mesh, in_specs=in_specs, out_specs=out_specs, check_vma=False
    )
```

```python
import functools

import jax
import jax.numpy as jnp
from jax import lax
from jax.experimental import pallas as pl
from jax.experimental.pallas import tpu as pltpu
from jax.sharding import PartitionSpec as P

MESH = pl.DeviceIdType.MESH
VMEM_LIMIT = 67_043_328
TOKEN_BYTES = 24 * 2**20
NT = (((1,), (1,)), ((), ()))
TN = (((0,), (0,)), ((), ()))
ROWS = 8


def dot_nt(a, b):
    return lax.dot_general(a, b, NT, preferred_element_type=jnp.float32)


def place():
    e = lax.axis_index("expert")
    c = lax.axis_index("etp")
    return e, c, e // 4, (e // 2) % 2, e % 2


def index(z, y, x):
    return z * 4 + y * 2 + x


def enter(groups, e, c):
    barrier = pltpu.get_barrier_semaphore()

    @pl.loop(1, groups)
    def _(i):
        pl.semaphore_signal(
            barrier, inc=1, device_id=(lax.rem(e + i, groups), c), device_id_type=MESH
        )

    pl.semaphore_signal(barrier, inc=1, device_id=(e, 1 - c), device_id_type=MESH)
    pl.semaphore_wait(barrier, groups)


def remote(src, dst, send, recv, expert, core):
    return pltpu.make_async_remote_copy(
        src_ref=src,
        dst_ref=dst,
        send_sem=send,
        recv_sem=recv,
        device_id=(expert, core),
        device_id_type=MESH,
    )


def one_hot(slot_row, capacity):
    tokens = slot_row.shape[1]
    at = lax.broadcasted_iota(jnp.int32, (capacity, tokens), 0).astype(jnp.float32)
    return jnp.where(slot_row == at, 1.0, 0.0)


def fused_kernel(
    nz, capacity, ra, rr,
    x_hbm, weights_ref, down_hbm, gate_hbm, up_hbm, saved_gate_hbm, saved_up_hbm,
    out_ref, part_out,
    own, other, mine, send, weights, slots_at, part, part_peer, part_sum,
    down, gate, up, work, hid, scale, saved_gate, saved_up, from_x, from_y, from_zc, from_zr,
    load_sem, saved_sem,
    asx, arx, asy, ary, asu, asd, arz, aru, ard, arr, acs, acr, sw, rw,
    rsx, rrx, rsy, rry, zcs, zcr, zrs, zrr, bcs, bcr, sp, rp, qs, qr, credit,
):
    e, c, z, y, x = place()
    groups = nz * 4
    per_group, hidden, model = down.shape
    tokens = weights.shape[2]
    half, features = own.shape[2:]
    width = 256
    pieces = hidden // width
    count = 4 * capacity
    beside, above = index(z, y, 1 - x), index(z, 1 - y, x)
    whole = pl.ds(0, half)
    tail = pl.ds(ra, half - ra)

    load_x = pltpu.make_async_copy(x_hbm, own.at[e], load_sem.at[0])
    load_x.start()
    loads = [
        pltpu.make_async_copy(src, dst, load_sem.at[i + 1])
        for i, (src, dst) in enumerate(((down_hbm, down), (gate_hbm, gate), (up_hbm, up)))
    ]

    def order(k):
        low = jnp.where(k <= z, z - k, k)
        back = nz - 1 - z
        high = jnp.where(k <= back, z + k, nz - 1 - k)
        return jnp.where(z < nz // 2, low, high)

    def passing(i):
        low = jnp.where(i < nz - 1 - z, z + 1 + i, nz - 2 - i)
        high = jnp.where(i < z, z - 1 - i, i + 1)
        return jnp.where(z < nz // 2, low, high)

    def load_saved(p):
        at = pl.ds(pl.multiple_of(p * count, count), count)
        return [
            pltpu.make_async_copy(saved_gate_hbm.at[:, at], saved_gate, saved_sem.at[0]),
            pltpu.make_async_copy(saved_up_hbm.at[:, at], saved_up, saved_sem.at[1]),
        ]

    weights[e] = weights_ref[e]
    enter(groups, e, c)

    def a_x(b, h, p, slot, rows):
        at = own.at[b, h, rows]
        return remote(at, at, asx.at[p, slot], arx.at[p, slot], beside, c)

    def a_y(b, h, p, slot, rows):
        at = own.at[b, h, rows]
        return remote(at, at, asy.at[p, slot], ary.at[p, slot], above, c)

    def a_z(p, h, up_way):
        at = own.at[index(p, y, x), h]
        sems = asu if up_way else asd
        return remote(at, at, sems.at[p, h], arz.at[p, h], e + 4 if up_way else e - 4, c)

    def others(p):
        return index(p, y, 1 - x), index(p, 1 - y, x), index(p, 1 - y, 1 - x)

    def a_r(p, j, up_way):
        at = own.at[others(p)[j], :, pl.ds(0, ra)]
        sems = aru if up_way else ard
        return remote(at, at, sems.at[p, j], arr.at[p, j], e + 4 if up_way else e - 4, c)

    def cross(b):
        return remote(own.at[b], other.at[b], acs.at[b], acr.at[b], e, 1 - c)

    def a_send(p, rows):
        b = index(p, y, x)
        a_x(b, 0, p, 0, rows).start()
        a_y(b, 1, p, 1, rows).start()
        a_x(b, 1, p, 1, rows).start()
        a_y(b, 0, p, 0, rows).start()

    def a_relay(p, rows):
        side, over, _ = others(p)
        a_x(side, 0, p, 0, rows).wait_recv()
        a_y(side, 0, p, 2, rows).start()
        a_y(over, 1, p, 1, rows).wait_recv()
        a_x(over, 1, p, 2, rows).start()

    def a_arrive(far):
        for h in range(2):
            @pl.when(z - far >= 0)
            def _():
                a_z(z - far, h, True).wait_recv()

                @pl.when(z < nz - 1)
                def _():
                    a_z(z - far, h, True).start()

            @pl.when(z + far < nz)
            def _():
                a_z(z + far, h, False).wait_recv()

                @pl.when(z > 0)
                def _():
                    a_z(z + far, h, False).start()

        @pl.when(far < nz)
        def _():
            after = order(far)
            a_send(after, tail)
            cross(index(after, y, x)).start()

    def a_spread(j):
        @pl.when(z < nz - 1)
        def _():
            a_r(z, j, True).start()

        @pl.when(z > 0)
        def _():
            a_r(z, j, False).start()

    def a_finish_own():
        side, over, corner = others(z)
        a_x(side, 1, z, 1, whole).wait_recv()
        a_spread(0)
        cross(side).start()
        a_y(over, 0, z, 0, whole).wait_recv()
        a_spread(1)
        cross(over).start()
        a_y(corner, 0, z, 2, whole).wait_recv()
        a_x(corner, 1, z, 2, whole).wait_recv()
        a_spread(2)
        cross(corner).start()

    def a_finish(k, p):
        @pl.when(z - k >= 0)
        def _():
            for j in range(3):
                a_r(z - k, j, True).wait_recv()

                @pl.when(z < nz - 1)
                def _():
                    a_r(z - k, j, True).start()

        @pl.when(z + k < nz)
        def _():
            for j in range(3):
                a_r(z + k, j, False).wait_recv()

                @pl.when(z > 0)
                def _():
                    a_r(z + k, j, False).start()

        side, over, corner = others(p)
        a_x(side, 1, p, 1, tail).wait_recv()
        cross(side).start()
        a_y(over, 0, p, 0, tail).wait_recv()
        cross(over).start()
        a_y(corner, 0, p, 2, tail).wait_recv()
        a_x(corner, 1, p, 2, tail).wait_recv()
        cross(corner).start()

    def tile(i):
        to = lax.rem(e + i, groups)
        return remote(weights_ref.at[to], weights.at[e], sw.at[i], rw.at[i], to, c)

    own_at = c * features
    other_at = (1 - c) * features

    def apart(first, second):
        none = jnp.zeros_like(first)
        upper = jnp.concatenate([first, none], axis=1)
        lower = jnp.concatenate([none, second], axis=1)
        return jnp.concatenate([upper, lower], axis=0).astype(jnp.bfloat16)

    def picks_of(b):
        slots = slots_at[b]
        return [one_hot(slots[l : l + 1], capacity) for l in range(per_group)]

    def gather(p, i, s, held):
        pick = apart(*[jnp.concatenate(picks_of(p * 4 + 2 * i + j), axis=0) for j in range(2)])
        block = held[pl.ds(p * 4 + 2 * i, 2)].reshape(2 * tokens, features)
        got = jnp.dot(pick, block, preferred_element_type=jnp.float32).astype(jnp.bfloat16)
        for j in range(2):
            for l in range(per_group):
                at = (j * per_group + l) * capacity
                to = l * count + (2 * i + j) * capacity
                work[s, pl.ds(to, capacity)] = got[at : at + capacity]

    def amounts(p, q):
        table = weights[p * 4 + q]
        picks = picks_of(p * 4 + q)
        for l in range(per_group):
            amount = jnp.sum(picks[l] * table[l : l + 1], axis=1, keepdims=True)
            scale[l, pl.ds(q * capacity, capacity)] = jnp.broadcast_to(amount, (capacity, 128))

    def hidden_grads(p, l, v):
        weight_part = jnp.zeros((count, 1), jnp.float32)
        at = pl.ds(pl.multiple_of(l * count, count), count)
        for j in range(pieces):
            cut = slice(j * width, (j + 1) * width)
            grad = dot_nt(work[0, at], down[l, cut, pl.ds(pl.multiple_of(own_at, 128), features)])
            grad = grad + dot_nt(work[1, at], down[l, cut, pl.ds(pl.multiple_of(other_at, 128), features)])
            gate_value = saved_gate[l, :, cut].astype(jnp.float32)
            up_value = saved_up[l, :, cut].astype(jnp.float32)
            sigmoid = jax.nn.sigmoid(gate_value)
            active = gate_value * sigmoid
            weight_part = weight_part + jnp.sum(grad * active * up_value, axis=1, keepdims=True)
            scaled = scale[l][:, :1] * grad
            grad_gate = scaled * up_value * sigmoid * (1.0 + gate_value * (1.0 - sigmoid))
            hid[v, l, :, cut] = grad_gate.astype(jnp.bfloat16)
            cut = slice(hidden + j * width, hidden + (j + 1) * width)
            hid[v, l, :, cut] = (scaled * active).astype(jnp.bfloat16)
        weight_part = weight_part.astype(jnp.bfloat16).astype(jnp.float32)
        for q in range(4):
            b = p * 4 + q
            pick = one_hot(slots_at[b, pl.ds(l, 1)], capacity)
            piece = weight_part[q * capacity : (q + 1) * capacity]
            part[b, pl.ds(l, 1)] = jnp.sum(pick * piece, axis=0, keepdims=True)

    def back_cross(p, q):
        t = jnp.where(p == z, 1, 0)
        return remote(send.at[q], other.at[p * 4 + q], bcs.at[t, q], bcr.at[t, q], e, 1 - c)

    def take(p):
        @pl.loop(0, 2)
        def _(i):
            gather(p, i, 0, own)

        @pl.loop(0, 4)
        def _(q):
            amounts(p, q)
            cross(p * 4 + q).wait_recv()

        @pl.loop(0, 2)
        def _(i):
            gather(p, i, 1, other)

        pl.semaphore_signal(credit.at[p], inc=1, device_id=(e, 1 - c), device_id_type=MESH)

    def grads(p, v):
        for copy in load_saved(p):
            copy.wait()

        @pl.loop(0, per_group)
        def _(l):
            hidden_grads(p, l, v)

    def products(s, start, v):
        @pl.loop(0, per_group)
        def _(l):
            rows = pl.ds(pl.multiple_of(start, 128), features)
            got = dot_nt(hid[v, l, :, :hidden], gate[l, rows])
            got = got + dot_nt(hid[v, l, :, hidden:], up[l, rows])
            got = got.astype(jnp.bfloat16)
            for q in range(4):
                at = q * per_group * capacity + l * capacity
                work[s, pl.ds(at, capacity)] = got[q * capacity : (q + 1) * capacity]

    def to_tokens(p, i, s):
        pick = apart(*[jnp.concatenate(picks_of(p * 4 + 2 * i + j), axis=0) for j in range(2)])
        size = 2 * per_group * capacity
        rows = pl.ds(pl.multiple_of(i * size, size), size)
        got = lax.dot_general(pick, work[s, rows], TN, preferred_element_type=jnp.float32)
        return got.astype(jnp.bfloat16).reshape(2, 2, half, features)

    def back_other(k, p, v):
        products(1, other_at, v)
        pl.semaphore_wait(credit.at[p], 1)

        @pl.loop(0, 2)
        def _(i):
            for j in range(2):
                @pl.when(k > 1)
                def _():
                    back_cross(last, 2 * i + j).wait_send()

            send[pl.ds(2 * i, 2)] = to_tokens(p, i, 1)
            for j in range(2):
                back_cross(p, 2 * i + j).start()

    def back_own(p, v):
        products(0, own_at, v)

        @pl.loop(0, 2)
        def _(i):
            got = to_tokens(p, i, 0)
            for j in range(2):
                b = p * 4 + 2 * i + j
                back_cross(p, 2 * i + j).wait_recv()
                mine[b] = (got[j].astype(jnp.float32) + other[b].astype(jnp.float32)).astype(jnp.bfloat16)

    low = pl.ds(0, rr)
    high = pl.ds(rr, half - rr)

    def add(b, h, rows, *terms):
        total = mine[b, h, rows].astype(jnp.float32)
        for term in terms:
            total = total + term.astype(jnp.float32)
        mine[b, h, rows] = total.astype(jnp.bfloat16)

    def r_x(b, h, t, slot, rows):
        dst = from_x.at[t, slot, pl.ds(0, rows.size)]
        return remote(mine.at[b, h, rows], dst, rsx.at[t, slot], rrx.at[t, slot], beside, c)

    def r_y(b, h, t, slot, rows):
        dst = from_y.at[t, slot, pl.ds(0, rows.size)]
        return remote(mine.at[b, h, rows], dst, rsy.at[t, slot], rry.at[t, slot], above, c)

    def landing(p, up_way):
        return p if up_way else jnp.where(p == z - 1, nz, p)

    links = 2 * (half // rr - 1)

    def piece(i):
        h, n = i // (half // rr - 1), lax.rem(i, half // rr - 1) + 1
        return h, pl.ds(pl.multiple_of(n * rr, rr), rr)

    def r_zc(p, i, up_way):
        t = landing(p, up_way)
        h, rows = piece(i)
        src = mine.at[index(p, y, x), h, rows]
        return remote(src, from_zc.at[t, i], zcs.at[p, i], zcr.at[t, i], e + 4 if up_way else e - 4, c)

    def r_zr(p, q, up_way):
        t = landing(p, up_way)
        src = mine.at[p * 4 + q, :, low]
        return remote(src, from_zr.at[t, q], zrs.at[p, q], zrr.at[t, q], e + 4 if up_way else e - 4, c)

    def got_zc(t, i):
        h, rows = piece(i)
        return remote(mine.at[e, h, rows], from_zc.at[t, i], zcs.at[0, i], zcr.at[t, i], e, 1 - c)

    def got_zr(t, q):
        return remote(mine.at[q, :, low], from_zr.at[t, q], zrs.at[0, q], zrr.at[t, q], e, 1 - c)

    def r_send(p, t, rows):
        side, over, corner = others(p)
        r_x(corner, 0, t, 0, rows).start()
        r_y(corner, 1, t, 0, rows).start()
        r_x(side, 0, t, 1, rows).start()
        r_y(over, 1, t, 2, rows).start()

    def r_relay(p, t, rows):
        side, over, _ = others(p)
        n = pl.ds(0, rows.size)
        r_x(side, 0, t, 0, rows).wait_recv()
        add(over, 0, rows, from_x[t, 0, n])
        r_y(over, 0, t, 1, rows).start()
        r_y(over, 1, t, 0, rows).wait_recv()
        add(side, 1, rows, from_y[t, 0, n])
        r_x(side, 1, t, 2, rows).start()

    def r_gather(p, t, rows):
        b = index(p, y, x)
        n = pl.ds(0, rows.size)
        for h in range(2):
            r_x(b, h, t, h + 1, rows).wait_recv()
            r_y(b, h, t, h + 1, rows).wait_recv()
            add(b, h, rows, from_x[t, h + 1, n], from_y[t, h + 1, n])

    def col_start(p):
        @pl.when((p > z) & (z == 0))
        def _():
            @pl.loop(0, links)
            def _(i):
                r_zc(p, i, True).start()

        @pl.when((p < z) & (z == nz - 1))
        def _():
            @pl.loop(0, links)
            def _(i):
                r_zc(p, i, False).start()

    def col_pass(p):
        def go(up_way):
            @pl.loop(0, links)
            def _(i):
                h, rows = piece(i)
                got_zc(p, i).wait_recv()
                add(index(p, y, x), h, rows, from_zc[p, i])
                r_zc(p, i, up_way).start()

        @pl.when((p > z) & (z > 0))
        def _():
            go(True)

        @pl.when((p < z) & (z < nz - 1))
        def _():
            go(False)

    def rows_start(p):
        @pl.when((p > z) & (z == 0))
        def _():
            for q in range(4):
                r_zr(p, q, True).start()

        @pl.when((p < z) & (z == nz - 1))
        def _():
            for q in range(4):
                r_zr(p, q, False).start()

    def rows_add(t, q, b):
        got_zr(t, q).wait_recv()
        for h in range(2):
            add(b, h, low, from_zr[t, q, h])

    def rows_pass(p):
        def go(up_way):
            @pl.loop(0, 4)
            def _(q):
                rows_add(p, q, p * 4 + q)
                r_zr(p, q, up_way).start()

        @pl.when((p > z) & (z > 0))
        def _():
            go(True)

        @pl.when((p < z) & (z < nz - 1))
        def _():
            go(False)

    def rows_final():
        @pl.when(z > 0)
        def _():
            @pl.loop(0, 4)
            def _(q):
                rows_add(z, q, z * 4 + q)

        @pl.when(z < nz - 1)
        def _():
            @pl.loop(0, 4)
            def _(q):
                rows_add(nz, q, z * 4 + q)

    @pl.loop(1, groups)
    def _(i):
        tile(i).start()

    load_x.wait()
    a_send(z, whole)
    for h in range(2):
        @pl.when(z < nz - 1)
        def _():
            a_z(z, h, True).start()

        @pl.when(z > 0)
        def _():
            a_z(z, h, False).start()

    cross(e).start()
    for copy in load_saved(z):
        copy.start()
    for copy in loads:
        copy.start()
    part[...] = jnp.zeros_like(part)
    a_relay(z, whole)
    a_arrive(1)

    @pl.loop(1, groups)
    def _(i):
        tile(i).wait_recv()

    named = (weights[...] > 0).astype(jnp.bfloat16).reshape(groups * ROWS, tokens)
    first = lax.broadcasted_iota(jnp.int32, (tokens, tokens), 0)
    second = lax.broadcasted_iota(jnp.int32, (tokens, tokens), 1)
    before = (first < second).astype(jnp.bfloat16)
    position = jnp.dot(named, before, preferred_element_type=jnp.float32)
    slots_at[...] = jnp.where(named > 0, position, -1.0).reshape(groups, ROWS, tokens)

    last = order(nz - 1)

    @pl.loop(0, nz + 1)
    def _(k):
        p = jnp.where(k < nz, order(k), z)
        v = jnp.where((k == 0) | (k == nz), 1, 0)

        @pl.when(k == 0)
        def _():
            a_finish_own()

        @pl.when((k > 0) & (k < nz))
        def _():
            a_finish(k, p)

        @pl.when(k < nz)
        def _():
            take(p)

        @pl.when(k + 1 < nz)
        def _():
            a_relay(order(k + 1), tail)

        @pl.when(k == 0)
        def _():
            for copy in loads:
                copy.wait()

        @pl.when(k < nz)
        def _():
            grads(p, v)

        @pl.when(k + 1 < nz)
        def _():
            for copy in load_saved(order(k + 1)):
                copy.start()

        @pl.when(k == 0)
        def _():
            a_arrive(2)

        @pl.when(k == nz - 1)
        def _():
            for i in range(1, nz - 2):
                r_gather(order(i), order(i), high)
                col_start(order(i))

        @pl.when(k == nz)
        def _():
            if nz > 2:
                rows_pass(passing(0))

        @pl.when(k > 0)
        def _():
            back_other(k, p, v)

        @pl.when((k > 0) & (k + 1 < nz))
        def _():
            a_arrive(k + 2)

        @pl.when(k == nz)
        def _():
            for i in range(max(nz - 2, 1), nz - 1):
                r_gather(order(i), order(i), high)
                col_start(order(i))

        @pl.when((k > 1) & (k < nz))
        def _():
            r_relay(order(k - 1), order(k - 1), high)

        @pl.when(k > 0)
        def _():
            back_own(p, v)

        @pl.when(k == nz)
        def _():
            r_relay(last, last, high)

        @pl.when(k > 0)
        def _():
            r_send(p, p, high)

        @pl.when((k > 0) & (k < nz))
        def _():
            rows_start(p)

    part_copy = remote(part, part_peer, sp, rp, e, 1 - c)
    part_copy.start()

    def part_tile(i):
        to = lax.rem(e + i, groups)
        return remote(part_sum.at[to], part_out.at[e], qs.at[i], qr.at[i], to, c)

    part_copy.wait()
    part_sum[...] = part[...] + part_peer[...]
    part_out[e] = part_sum[e]

    @pl.loop(1, groups)
    def _(i):
        part_tile(i).start()

    rows_pass(passing(1 if nz > 2 else 0))
    r_gather(last, last, high)
    col_start(last)
    for i in range(2, nz - 1):
        rows_pass(passing(i))
    rows_final()
    r_send(z, nz, low)
    r_relay(z, z, high)
    for i in range(nz - 2):
        col_pass(passing(i))
    r_relay(z, nz, low)
    col_pass(passing(nz - 2))
    r_gather(z, z, high)
    r_gather(z, nz, low)

    at_home = index(z, y, x)
    out_ref[...] = mine[at_home]

    def col_final(t):
        @pl.loop(0, links)
        def _(i):
            h, rows = piece(i)
            got_zc(t, i).wait_recv()
            total = out_ref[h, rows].astype(jnp.float32) + from_zc[t, i].astype(jnp.float32)
            out_ref[h, rows] = total.astype(jnp.bfloat16)

    @pl.when(z > 0)
    def _():
        col_final(z)

    @pl.when(z < nz - 1)
    def _():
        col_final(nz)

    @pl.loop(1, groups)
    def _(i):
        tile(i).wait_send()
        part_tile(i).wait()

    def sent_xy(p, rows):
        for slot in range(3):
            a_x(e, 0, p, slot, rows).wait_send()
            a_y(e, 0, p, slot, rows).wait_send()

    sent_xy(z, whole)
    for slot in range(3):
        r_x(e, 0, nz, slot, low).wait_send()
        r_y(e, 0, nz, slot, low).wait_send()

    @pl.loop(0, nz)
    def _(p):
        @pl.when(p != z)
        def _():
            sent_xy(p, tail)

        for slot in range(3):
            r_x(e, 0, p, slot, high).wait_send()
            r_y(e, 0, p, slot, high).wait_send()

        @pl.when((p <= z) & (z < nz - 1))
        def _():
            for h in range(2):
                a_z(p, h, True).wait_send()
            for j in range(3):
                a_r(p, j, True).wait_send()

        @pl.when((p >= z) & (z > 0))
        def _():
            for h in range(2):
                a_z(p, h, False).wait_send()
            for j in range(3):
                a_r(p, j, False).wait_send()

        @pl.when((p > z) & (z < nz - 1))
        def _():
            for i in range(links):
                r_zc(p, i, True).wait_send()
            for q in range(4):
                r_zr(p, q, True).wait_send()

        @pl.when((p < z) & (z > 0))
        def _():
            for i in range(links):
                r_zc(p, i, False).wait_send()
            for q in range(4):
                r_zr(p, q, False).wait_send()

    @pl.loop(0, groups)
    def _(b):
        cross(b).wait_send()

    @pl.loop(0, 4)
    def _(q):
        back_cross(z, q).wait_send()


def with_kernel(
    grad_out, combine, expert_ids, saved_gate, saved_up, gate_weight, up_weight, down_weight
):
    groups = lax.axis_size("expert")
    nz = groups // 4
    per_group, model, hidden = gate_weight.shape
    tokens, features = grad_out.shape
    capacity = saved_gate.shape[0] // groups
    experts = groups * per_group
    half = tokens // 2
    ra = half // 64 * 16
    rr = half // 64 * 16
    links = 2 * (half // rr - 1)
    chosen = expert_ids[:, :, None] == jnp.arange(experts, dtype=jnp.int32)[None, None, :]
    weights = jnp.sum(jnp.where(chosen, combine[:, :, None].astype(jnp.float32), 0.0), axis=1)
    weights = weights.reshape(tokens, groups, per_group).transpose(1, 2, 0)
    weights = jnp.pad(weights, ((0, 0), (0, ROWS - per_group), (0, 0)))
    gate_value = saved_gate.transpose(1, 0, 2)
    up_value = saved_up.transpose(1, 0, 2)
    vmem = pl.BlockSpec(memory_space=pltpu.VMEM)
    hbm = pl.BlockSpec(memory_space=pltpu.HBM)
    bf16, f32 = jnp.bfloat16, jnp.float32
    dma = pltpu.SemaphoreType.DMA
    table = pltpu.VMEM((groups, ROWS, tokens), f32)
    blocks = pltpu.VMEM((groups, 2, half, features), bf16)
    count = 4 * capacity
    grad_tokens, parts = pl.pallas_call(
        functools.partial(fused_kernel, nz, capacity, ra, rr),
        name="experts",
        out_shape=(
            jax.ShapeDtypeStruct((2, half, features), bf16),
            jax.ShapeDtypeStruct((groups, ROWS, tokens), f32),
        ),
        in_specs=[hbm, vmem, hbm, hbm, hbm, hbm, hbm],
        out_specs=(vmem, vmem),
        scratch_shapes=[
            blocks, blocks, blocks,
            pltpu.VMEM((4, 2, half, features), bf16),
            table, table, table, table, table,
            pltpu.VMEM((per_group, hidden, model), bf16),
            pltpu.VMEM((per_group, model, hidden), bf16),
            pltpu.VMEM((per_group, model, hidden), bf16),
            pltpu.VMEM((2, per_group * count, features), bf16),
            pltpu.VMEM((2, per_group, count, 2 * hidden), bf16),
            pltpu.VMEM((per_group, count, 128), f32),
            pltpu.VMEM((per_group, count, hidden), bf16),
            pltpu.VMEM((per_group, count, hidden), bf16),
            pltpu.VMEM((nz + 1, 3, half - rr, features), bf16),
            pltpu.VMEM((nz + 1, 3, half - rr, features), bf16),
            pltpu.VMEM((nz + 1, links, rr, features), bf16),
            pltpu.VMEM((nz + 1, 4, 2, rr, features), bf16),
            dma((4,)), dma((2,)),
            dma((nz, 3)), dma((nz, 3)), dma((nz, 3)), dma((nz, 3)),
            dma((nz, 2)), dma((nz, 2)), dma((nz, 2)),
            dma((nz, 3)), dma((nz, 3)), dma((nz, 3)),
            dma((groups,)), dma((groups,)), dma((groups,)), dma((groups,)),
            dma((nz + 1, 3)), dma((nz + 1, 3)), dma((nz + 1, 3)), dma((nz + 1, 3)),
            dma((nz, links)), dma((nz + 1, links)), dma((nz, 4)), dma((nz + 1, 4)),
            dma((2, 4)), dma((2, 4)), dma(()), dma(()), dma((groups,)), dma((groups,)),
            pltpu.SemaphoreType.REGULAR((nz,)),
        ],
        compiler_params=pltpu.CompilerParams(
            collective_id=0, has_side_effects=True, vmem_limit_bytes=VMEM_LIMIT
        ),
    )(grad_out.reshape(2, half, features), weights, down_weight, gate_weight, up_weight, gate_value, up_value)
    parts = parts[:, :per_group].transpose(2, 0, 1).reshape(tokens, 1, experts)
    grad_combine = jnp.sum(jnp.where(chosen, parts, 0.0), axis=2).astype(jnp.bfloat16)
    return grad_tokens.reshape(tokens, features), grad_combine


def with_collectives(
    grad_out, combine, expert_ids, saved_gate, saved_up, gate_weight, up_weight, down_weight
):
    groups = lax.axis_size("expert")
    per_group = gate_weight.shape[0]
    tokens = grad_out.shape[0]
    capacity = saved_gate.shape[0] // groups
    hidden = saved_gate.shape[2]
    experts = groups * per_group
    chosen = expert_ids[:, :, None] == jnp.arange(experts, dtype=jnp.int32)[None, None, :]
    weights = jnp.sum(jnp.where(chosen, combine[:, :, None].astype(jnp.float32), 0.0), axis=1)
    weights = weights.astype(jnp.bfloat16).reshape(tokens, groups, per_group)
    weights = lax.all_to_all(
        weights.transpose(1, 2, 0), "expert", split_axis=0, concat_axis=0, tiled=True
    )
    rows = lax.all_gather(grad_out, "expert", axis=0, tiled=True)
    rows = lax.all_gather(rows, "etp", axis=1, tiled=True)
    rows = rows.reshape(groups, tokens, -1)
    named = (weights > 0).astype(jnp.float32)
    position = jnp.cumsum(named, axis=2) - named
    slot = jnp.where(named > 0, position, -1.0)
    select = slot[:, :, None, :] == jnp.arange(capacity, dtype=jnp.float32)[None, None, :, None]
    scale = jnp.sum(jnp.where(select, weights[:, :, None, :].astype(jnp.float32), 0.0), axis=3)
    scale = scale.transpose(1, 0, 2)[..., None]
    select = select.astype(jnp.bfloat16)
    slot_rows = jnp.einsum(
        "blct,btd->lbcd", select, rows, preferred_element_type=jnp.bfloat16
    )
    grad_hidden = jnp.einsum(
        "lbcd,lfd->lbcf", slot_rows, down_weight, preferred_element_type=jnp.float32
    )
    gate_value = saved_gate.reshape(groups, capacity, per_group, hidden).transpose(2, 0, 1, 3)
    up_value = saved_up.reshape(groups, capacity, per_group, hidden).transpose(2, 0, 1, 3)
    gate_value = gate_value.astype(jnp.float32)
    up_value = up_value.astype(jnp.float32)
    gate_sigmoid = jax.nn.sigmoid(gate_value)
    activated = gate_value * gate_sigmoid
    weight_part = jnp.sum(grad_hidden * activated * up_value, axis=3)
    scaled = scale * grad_hidden
    grad_gate = (
        scaled * up_value * gate_sigmoid * (1.0 + gate_value * (1.0 - gate_sigmoid))
    ).astype(jnp.bfloat16)
    grad_up = (scaled * activated).astype(jnp.bfloat16)
    weight_tok = jnp.einsum(
        "blct,lbc->blt", select, weight_part.astype(jnp.bfloat16),
        preferred_element_type=jnp.float32,
    ).astype(jnp.bfloat16)
    weight_tok = lax.psum(weight_tok, "etp")
    weight_tok = lax.all_to_all(weight_tok, "expert", split_axis=0, concat_axis=0, tiled=True)
    weight_tok = weight_tok.transpose(2, 0, 1).reshape(tokens, 1, experts)
    grad_combine = jnp.sum(
        jnp.where(chosen, weight_tok.astype(jnp.float32), 0.0), axis=2
    ).astype(jnp.bfloat16)
    partial = jnp.einsum(
        "lbcf,ldf->lbcd", grad_gate, gate_weight, preferred_element_type=jnp.float32
    )
    partial = partial + jnp.einsum(
        "lbcf,ldf->lbcd", grad_up, up_weight, preferred_element_type=jnp.float32
    )
    partial = jnp.einsum(
        "blct,lbcd->btd", select, partial.astype(jnp.bfloat16),
        preferred_element_type=jnp.float32,
    ).astype(jnp.bfloat16)
    partial = partial.reshape(groups * tokens, -1)
    partial = lax.psum_scatter(partial, "etp", scatter_dimension=1, tiled=True)
    grad_tokens = lax.psum_scatter(partial, "expert", scatter_dimension=0, tiled=True)
    return (grad_tokens, grad_combine)


def on_device(grad_out, *rest):
    groups = lax.axis_size("expert")
    held = 4 * groups * grad_out.size
    if groups % 4 == 0 and lax.axis_size("etp") == 2 and held <= TOKEN_BYTES:
        return with_kernel(grad_out, *rest)
    return with_collectives(grad_out, *rest)


def solution(mesh):
    in_specs = (
        P("expert", "etp"),
        P("expert", None),
        P("expert", None),
        P(None, "expert", "etp"),
        P(None, "expert", "etp"),
        P("expert", None, "etp"),
        P("expert", None, "etp"),
        P("expert", "etp", None),
    )
    out_specs = (P("expert", "etp"), P("expert", None))
    return jax.shard_map(
        on_device, mesh=mesh, in_specs=in_specs, out_specs=out_specs, check_vma=False
    )
```
